32 devices in a mesh: row: 4 (over z), col: 8 (over y, x, core).
Axes of the slice: x: 2, y: 2, z: 4, core: 2. Of those that a mesh axis runs over, the one named last changes fastest.
Arguments:
- a_matrix: float32 [8192, 8192], P('row', 'col'), may hold values from -14 to 30, as said below
- b_matrix: float32 [4096, 4096], P('row', 'col'), may hold values from -14 to 30, as said below
- c_matrix: float32 [8192, 4096], P('row', 'col'), may hold values from -6 to 6
Outputs:
- a_swept: float32 [8192, 8192], P('row', 'col')
- c_swept: float32 [8192, 4096], P('row', 'col')
- b_next: float32 [4096, 4096], P('row', 'col')
The draws below stay inside these ranges and needn't reach their ends.
Inputs may be any that keep to these rules, and one draw needn't show every extreme that they name: `a_matrix`: symmetric positive definite; its smallest eigenvalue is at least 1. `b_matrix`: symmetric positive definite; its smallest eigenvalue is at least 1.
All inputs are finite; a program needn't handle non-finite values. Where the reference program divides by a largest or mean magnitude, that divisor is 1e-20 or more.
Results may differ from the reference program's by a relative error of at most 0.00012.
Values sent between devices are 32-bit elements; how exact they have to be, the bound alone decides.
A program may use at most 128 MiB of HBM per device.

```python
import math
import jax
import jax.numpy as jnp
from jax import lax

NA = 8192
NB = 4096
PANEL = 256
PIVOT_ITERS = 6
STEPS_A = 2
STEPS_B = 16


def definite(key, order):
    first_key, second_key, third_key = jax.random.split(key, 3)
    inner = order // 4
    limit = math.sqrt(3.0)
    factor = jax.random.uniform(first_key, (order, inner), jnp.float32, -limit, limit)
    spread = math.log(2.0)
    coupling = jnp.dot(factor, factor.T, precision=lax.Precision.HIGHEST, preferred_element_type=jnp.float32) / inner
    block_scale = jnp.exp(jax.random.uniform(second_key, (16,), jnp.float32, 0.0, 0.5 * spread))
    block_scale = jnp.repeat(block_scale, order // 16)
    row_scale = block_scale * jnp.exp(jax.random.uniform(third_key, (order,), jnp.float32, 0.0, 0.5 * spread))
    identity = jnp.eye(order, dtype=jnp.float32)
    core = identity + 0.25 * coupling
    return row_scale[:, None] * core * row_scale[None, :]


def draw_a_matrix(key, part):
    return definite(jax.random.fold_in(key, 11), NA)


def draw_b_matrix(key, part):
    return definite(jax.random.fold_in(key, 23), NB)


def steps_of(key, extent, cuts, low, high):
    loudness = 1.0
    for axis_at, shards_of in cuts:
        steps = jax.random.uniform(jax.random.fold_in(jax.random.fold_in(key, 6), axis_at), (shards_of,), jnp.float32, low / len(cuts), high / len(cuts))
        loudness = loudness * jnp.repeat(jnp.exp(steps), extent[axis_at] // shards_of).reshape((-1,) + (1,) * (len(extent) - 1 - axis_at))
    return loudness


def scatter_about(rng, extent, deviation, bound, pieces=(), held_as=jnp.bfloat16):
    gain = steps_of(rng, extent, pieces, -0.22, 0.18) if pieces else 1.0
    values = jax.random.normal(rng, extent, jnp.float32) * deviation * gain
    return jnp.minimum(jnp.maximum(values, -bound), bound).astype(held_as)


def setup_inputs(seed: int = 0) -> dict:
    keys = jax.random.split(jax.random.key(seed), 4)
    a_matrix = draw_a_matrix(jax.random.fold_in(keys[3], 71), 0)
    b_matrix = draw_b_matrix(jax.random.fold_in(keys[3], 71), 0)
    c_matrix = scatter_about(keys[2], (NA, NB), 1.0, 6.0, ((0, 4), (1, 8)), jnp.float32)
    return dict(a_matrix=a_matrix, b_matrix=b_matrix, c_matrix=c_matrix)


EXACT = lax.Precision.HIGHEST

def pivot_inverse(pivot):
    order = pivot.shape[0]
    scaling = 1.0 / jnp.sqrt(jnp.diagonal(pivot))
    unit = pivot * scaling[:, None] * scaling[None, :]
    ceiling = jnp.max(lax.optimization_barrier(jnp.sum(jnp.abs(unit), axis=1)))
    approx = jnp.eye(order, dtype=jnp.float32) / ceiling
    for turn in range(PIVOT_ITERS):
        product = jnp.dot(unit, approx, precision=EXACT, preferred_element_type=jnp.float32)
        approx = 2.0 * approx - jnp.dot(approx, product, precision=EXACT, preferred_element_type=jnp.float32)
    return approx * scaling[:, None] * scaling[None, :]

def sweep(matrix, other, count):
    order = matrix.shape[0]
    index = jnp.arange(order, dtype=jnp.int32)
    for step in range(count):
        first = step * PANEL
        eye_rows = (index[:, None] == first + jnp.arange(PANEL, dtype=jnp.int32)[None, :]).astype(jnp.float32)
        inverse = pivot_inverse(matrix[first:first + PANEL, first:first + PANEL])
        solved = jnp.dot(matrix[:, first:first + PANEL] - eye_rows, inverse, precision=EXACT, preferred_element_type=jnp.float32)
        rows = matrix[first:first + PANEL, :]
        updated = matrix - jnp.dot(solved, rows, precision=EXACT, preferred_element_type=jnp.float32)
        matrix = updated.at[:, first:first + PANEL].set(eye_rows - solved)
        if other is not None:
            other = other - jnp.dot(solved, other[first:first + PANEL, :], precision=EXACT, preferred_element_type=jnp.float32)
    return (matrix, other)

def reference(a_matrix, b_matrix, c_matrix):
    a_swept, c_swept = sweep(a_matrix, c_matrix, STEPS_A)
    b_inverse, unused = sweep(b_matrix, None, STEPS_B)
    b_squares = jnp.sum(b_matrix * b_matrix)
    inv_squares = jnp.sum(b_inverse * b_inverse)
    scale = jnp.sqrt(jnp.sqrt(inv_squares / b_squares))
    b_next = 0.5 * (scale * b_matrix + b_inverse / scale)
    return (a_swept, c_swept, b_next)
```

```python
import functools

import jax
import jax.numpy as jnp
from jax import lax
from jax.experimental import pallas as pl
from jax.experimental.pallas import tpu as pltpu
from jax.sharding import PartitionSpec as P

PANEL = 256
PIVOT_ITERS = 6
STEPS_A = 2
STEPS_B = 16

EXACT = lax.Precision.HIGHEST
SPLIT = lax.Precision.HIGH


def dot(x, y, precision):
    return jnp.dot(x, y, precision=precision, preferred_element_type=jnp.float32)


def tree(value, axis, source, masks):
    apart = lax.axis_index(axis) ^ source
    holders = [source]
    seen = 0
    for mask in masks:
        pairs = [(holder, holder ^ mask) for holder in holders]
        arrived = lax.ppermute(value, axis, pairs)
        value = jnp.where((apart & ~seen) == 0, value, arrived)
        holders = holders + [target for _, target in pairs]
        seen |= mask
    return value


def spread(value, axis, source):
    size = lax.axis_size(axis)
    if size & (size - 1):
        kept = jnp.where(lax.axis_index(axis) == source, value, 0).astype(value.dtype)
        return lax.psum(kept, axis)
    masks = [1 << bit for bit in reversed(range(size.bit_length() - 1))]
    if len(masks) < 3:
        return tree(value, axis, source, masks)
    half = value.shape[0] // 2
    crossed = [masks[1], masks[0]] + masks[2:]
    return jnp.concatenate(
        [tree(value[:half], axis, source, masks), tree(value[half:], axis, source, crossed)], 0
    )


def pivot_inverse(pivot, precision):
    order = pivot.shape[0]
    down = lax.broadcasted_iota(jnp.int32, (order, order), 0)
    across = lax.broadcasted_iota(jnp.int32, (order, order), 1)
    eye = (down == across).astype(jnp.float32)
    kept = pivot * eye
    tall = 1.0 / jnp.sqrt(jnp.sum(kept, axis=1, keepdims=True))
    wide = 1.0 / jnp.sqrt(jnp.sum(kept, axis=0, keepdims=True))
    unit = pivot * tall * wide
    ceiling = jnp.max(jnp.sum(jnp.abs(unit), axis=1, keepdims=True), axis=0, keepdims=True)
    power = eye - unit / ceiling
    total = eye + power
    power = dot(power, power, precision)
    for turn in range(1, PIVOT_ITERS - 1):
        both = dot(power, jnp.concatenate([power, total], 1), precision)
        total = total + both[:, order:]
        power = both[:, :order]
    total = total + dot(power, total, precision)
    return total / ceiling * tall * wide


def lookup(index, table):
    value = jnp.int32(table[0])
    for place in range(1, len(table)):
        value = jnp.where(index == place, jnp.int32(table[place]), value)
    return value


class Plan:
    def __init__(self, mesh):
        self.rows = mesh.shape["row"]
        self.cols = mesh.shape["col"]
        line = list(mesh.devices.reshape(self.rows, self.cols)[0])
        at = [tuple(getattr(device, "coords", (place, 0, 0))) for place, device in enumerate(line)]
        paired = self.cols % 2 == 0 and all(at[2 * i] == at[2 * i + 1] for i in range(self.cols // 2))
        self.cores = 2 if paired else 1
        chips = at[:: self.cores]
        order = sorted(range(len(chips)), key=lambda i: (chips[i][1], chips[i][0] * (-1) ** chips[i][1]))
        count = len(order)
        self.chips = count
        self.after = [0] * count
        self.before = [0] * count
        for place, chip in enumerate(order):
            self.after[chip] = order[(place + 1) % count]
            self.before[chip] = order[(place - 1) % count]


def sweep_kernel(plan, steps, b_ref, o_ref, m, w, r, x, t, in_sem, row_recv, row_up, row_down, w_recv, w_ring, w_pair):
    tiles, height, _ = m.shape
    blocks = height // PANEL
    half = PANEL // 2
    me_row = lax.axis_index("row")
    me_col = lax.axis_index("col")
    cores = plan.cores
    chip = me_col // cores
    core = me_col % cores
    pair = chip * cores + (cores - 1 - core)

    def to_row(place):
        return {"row": place, "col": me_col}

    def to_col(place):
        return {"row": me_row, "col": place}

    nexts = [lookup(chip, plan.after), lookup(chip, plan.before)]
    ring_to = [nexts[h] * cores + (core if cores == 2 else 0) for h in range(2)]

    loads = [
        pltpu.make_async_copy(b_ref.at[:, pl.ds(j * PANEL, PANEL)], m.at[j], in_sem.at[j]) for j in range(tiles)
    ]
    for load in loads:
        load.start()

    barrier = pltpu.get_barrier_semaphore()

    def greet(target):
        pl.semaphore_signal(barrier, inc=1, device_id=target, device_id_type=pl.DeviceIdType.MESH)

    @pl.when(me_row > 0)
    def _():
        greet(to_row(me_row - 1))

    @pl.when(me_row < plan.rows - 1)
    def _():
        greet(to_row(me_row + 1))

    for h in range(2):
        greet(to_col(ring_to[h]))
    if cores == 2:
        greet(to_col(pair))
    inner = jnp.where(me_row > 0, 1, 0) + jnp.where(me_row < plan.rows - 1, 1, 0)
    pl.semaphore_wait(barrier, inner + 2 + (cores - 1))
    for load in loads:
        load.wait()

    def row_copy(p, i, up):
        j = (p + i) % tiles
        return pltpu.make_async_remote_copy(
            src_ref=r.at[p, j],
            dst_ref=r.at[p, j],
            send_sem=(row_up if up else row_down).at[p, i],
            recv_sem=row_recv.at[p, i],
            device_id=to_row(me_row + 1 if up else me_row - 1),
            device_id_type=pl.DeviceIdType.MESH,
        )

    def piece(p, h, i):
        start = ((p + 1 + i) % blocks) * PANEL + h * half
        return pl.ds(pl.multiple_of(start, half), half)

    def ring_copy(p, h, i):
        return pltpu.make_async_remote_copy(
            src_ref=w.at[p, piece(p, h, i)],
            dst_ref=w.at[p, piece(p, h, i)],
            send_sem=w_ring.at[p, h, i],
            recv_sem=w_recv.at[p, h, i],
            device_id=to_col(ring_to[h] if isinstance(h, int) else pair),
            device_id_type=pl.DeviceIdType.MESH,
        )

    def pair_copy(p, h, i):
        return pltpu.make_async_remote_copy(
            src_ref=w.at[p, piece(p, h, i)],
            dst_ref=w.at[p, piece(p, h, i)],
            send_sem=w_pair.at[p, h, i],
            recv_sem=w_recv.at[p, h, i],
            device_id=to_col(pair),
            device_id_type=pl.DeviceIdType.MESH,
        )

    def row_root(p):
        return p // blocks

    def col_root(p):
        return p // tiles

    def sends_up(p):
        return (me_row >= row_root(p)) & (me_row < plan.rows - 1)

    def sends_down(p):
        return (me_row <= row_root(p)) & (me_row > 0)

    def row_sends(p, i, act):
        @pl.when(sends_up(p))
        def _():
            act(row_copy(p, i, True))

        @pl.when(sends_down(p))
        def _():
            act(row_copy(p, i, False))

    def carries(h):
        return True if cores == 1 else core == h

    def ring_on(p, h):
        return carries(h) & (nexts[h] != col_root(p) // cores)

    def pair_on(p, h):
        home = chip == col_root(p) // cores
        owner = me_col == col_root(p)
        return owner | (jnp.logical_not(home) & carries(h))

    def w_sends(p, h, i, act):
        @pl.when(ring_on(p, h))
        def _():
            act(ring_copy(p, h, i))

        if cores == 2:

            @pl.when(pair_on(p, h))
            def _():
                act(pair_copy(p, h, i))

    def start(copy):
        copy.start()

    def take_carried(p, which):
        @pl.when(me_col != col_root(p))
        def _():
            for i in which:
                for h in range(2):
                    if cores == 2:

                        @pl.when(core == h)
                        def _():
                            ring_copy(p, h, i).wait_recv()
                            w_sends(p, h, i, start)

                    else:
                        ring_copy(p, h, i).wait_recv()
                        w_sends(p, h, i, start)

    def take_other(p, which):
        if cores == 2:

            @pl.when(me_col != col_root(p))
            def _():
                for i in which:
                    ring_copy(p, 1 - core, i).wait_recv()

    def block(p):
        return pl.ds(pl.multiple_of((p % blocks) * PANEL, PANEL), PANEL)

    def make_rows(p):
        for j in range(tiles):
            fresh = m[j, block(p), :]

            @pl.when(p == 0)
            def _():
                r[p, j] = fresh

            @pl.when(p > 0)
            def _():
                q = jnp.maximum(p - 1, 0)
                step = w[q, block(p), :]
                swept = (me_col == col_root(q)) & (q % tiles == j)

                @pl.when(swept)
                def _():
                    r[p, j] = -step

                @pl.when(jnp.logical_not(swept))
                def _():
                    r[p, j] = fresh - dot(step, r[q, j], SPLIT)

    def make_w(p):
        j = p % tiles

        @pl.when(p == 0)
        def _():
            t[...] = m[j]

        @pl.when(p > 0)
        def _():
            q = jnp.maximum(p - 1, 0)
            t[...] = m[j] - dot(w[q], r[q, j], SPLIT)

        @pl.when(me_row == row_root(p))
        def _():
            t[block(p), :] = t[block(p), :] - unit()

        w[p] = dot(t[...], x[...], SPLIT)

    def unit():
        down = lax.broadcasted_iota(jnp.int32, (PANEL, PANEL), 0)
        across = lax.broadcasted_iota(jnp.int32, (PANEL, PANEL), 1)
        return (down == across).astype(jnp.float32)

    def update(q):
        for j in range(tiles):
            swept = (me_col == col_root(q)) & (q % tiles == j)

            @pl.when(swept)
            def _():
                m[j] = -w[q]

                @pl.when(me_row == row_root(q))
                def _():
                    m[j, block(q), :] = unit() - w[q, block(q), :]

            @pl.when(jnp.logical_not(swept))
            def _():
                m[j] = m[j] - dot(w[q], r[q, j], SPLIT)

    def step(p, carry):
        root = me_row == row_root(p)
        owner = me_col == col_root(p)
        q = jnp.maximum(p - 1, 0)

        @pl.when(jnp.logical_not(root))
        def _():
            for i in range(tiles):
                row_copy(p, i, True).wait_recv()
                row_sends(p, i, start)

        @pl.when(p > 0)
        def _():
            take_carried(q, range(blocks))
            take_other(q, range(1))

        @pl.when(root)
        def _():
            make_rows(p)
            for i in range(tiles):
                row_sends(p, i, start)

        @pl.when(owner)
        def _():
            x[...] = pivot_inverse(r[p, p % tiles], SPLIT)

        @pl.when(p > 0)
        def _():
            take_other(q, range(1, blocks))

        @pl.when(owner)
        def _():
            make_w(p)
            for i in range(blocks):
                for h in range(2):
                    w_sends(p, h, i, start)

        @pl.when(p > 0)
        def _():
            update(q)

        return carry

    lax.fori_loop(0, steps, step, 0)
    take_carried(steps - 1, range(blocks))
    take_other(steps - 1, range(blocks))
    update(steps - 1)

    stores = [
        pltpu.make_async_copy(m.at[j], o_ref.at[:, pl.ds(j * PANEL, PANEL)], in_sem.at[j]) for j in range(tiles)
    ]
    for store in stores:
        store.start()

    def drain(p, carry):
        for i in range(tiles):
            row_sends(p, i, lambda copy: copy.wait_send())
        for i in range(blocks):
            for h in range(2):
                w_sends(p, h, i, lambda copy: copy.wait_send())
        return carry

    lax.fori_loop(0, steps, drain, 0)
    for store in stores:
        store.wait()


def sweep_b(plan, matrix):
    height, width = matrix.shape
    tiles = width // PANEL
    blocks = height // PANEL
    steps = STEPS_B
    return pl.pallas_call(
        functools.partial(sweep_kernel, plan, steps),
        out_shape=jax.ShapeDtypeStruct((height, width), jnp.float32),
        in_specs=[pl.BlockSpec(memory_space=pl.ANY)],
        out_specs=pl.BlockSpec(memory_space=pl.ANY),
        scratch_shapes=[
            pltpu.VMEM((tiles, height, PANEL), jnp.float32),
            pltpu.VMEM((steps, height, PANEL), jnp.float32),
            pltpu.VMEM((steps, tiles, PANEL, PANEL), jnp.float32),
            pltpu.VMEM((PANEL, PANEL), jnp.float32),
            pltpu.VMEM((height, PANEL), jnp.float32),
            pltpu.SemaphoreType.DMA((tiles,)),
            pltpu.SemaphoreType.DMA((steps, tiles)),
            pltpu.SemaphoreType.DMA((steps, tiles)),
            pltpu.SemaphoreType.DMA((steps, tiles)),
            pltpu.SemaphoreType.DMA((steps, 2, blocks)),
            pltpu.SemaphoreType.DMA((steps, 2, blocks)),
            pltpu.SemaphoreType.DMA((steps, 2, blocks)),
        ],
        compiler_params=pltpu.CompilerParams(
            collective_id=0, has_side_effects=True, vmem_limit_bytes=48 * 1024 * 1024
        ),
        name="sweep_b",
    )(matrix)


def frame(matrix, first):
    local_rows = matrix.shape[0]
    row_place = lax.axis_index("row")
    col_place = lax.axis_index("col")
    global_rows = row_place * local_rows + jnp.arange(local_rows, dtype=jnp.int32)
    eye_rows = (global_rows[:, None] == first + jnp.arange(PANEL, dtype=jnp.int32)[None, :]).astype(
        jnp.float32
    )
    return (eye_rows, col_place)


def finish(matrix, solved, rows, first, eye_rows, col_place):
    local_cols = matrix.shape[1]
    offset = first % local_cols
    root_col = first // local_cols
    updated = matrix - jnp.dot(solved, rows, precision=SPLIT, preferred_element_type=jnp.float32)
    current = updated[:, offset : offset + PANEL]
    placed = jnp.where(col_place == root_col, eye_rows - solved, current)
    return updated.at[:, offset : offset + PANEL].set(placed)


def a_step(matrix, other, step):
    local_rows, local_cols = matrix.shape
    other_cols = other.shape[1]
    first = step * PANEL
    root_row = first // local_rows
    row_offset = first % local_rows
    root_col = first // local_cols
    col_offset = first % local_cols
    eye_rows, col_place = frame(matrix, first)
    rows = matrix[row_offset : row_offset + PANEL, :]
    other_rows = other[row_offset : row_offset + PANEL, :]
    column = spread(matrix[:, col_offset : col_offset + PANEL], "col", root_col)
    pivot = column[row_offset : row_offset + PANEL, :]
    joined = spread(jnp.concatenate([rows, other_rows, pivot], 1), "row", root_row)
    rows = joined[:, :local_cols]
    other_rows = joined[:, local_cols : local_cols + other_cols]
    pivot = joined[:, local_cols + other_cols :]
    solved = jnp.dot(
        column - eye_rows, pivot_inverse(pivot, EXACT), precision=EXACT, preferred_element_type=jnp.float32
    )
    new_matrix = finish(matrix, solved, rows, first, eye_rows, col_place)
    new_other = other - jnp.dot(
        solved, other_rows, precision=SPLIT, preferred_element_type=jnp.float32
    )
    return (new_matrix, new_other)


def body(plan, a_matrix, b_matrix, c_matrix):
    b_local = jnp.sum(b_matrix * b_matrix)
    a_swept, c_swept = (a_matrix, c_matrix)
    for step in range(STEPS_A):
        a_swept, c_swept = a_step(a_swept, c_swept, step)
    b_inverse = sweep_b(plan, b_matrix)
    inv_local = jnp.sum(b_inverse * b_inverse)
    b_squares, inv_squares = lax.psum((b_local, inv_local), ("row", "col"))
    scale = jnp.sqrt(jnp.sqrt(inv_squares / b_squares))
    b_next = 0.5 * (scale * b_matrix + b_inverse / scale)
    return (a_swept, c_swept, b_next)


def solution(mesh):
    return jax.shard_map(
        functools.partial(body, Plan(mesh)),
        mesh=mesh,
        in_specs=(P("row", "col"), P("row", "col"), P("row", "col")),
        out_specs=(P("row", "col"), P("row", "col"), P("row", "col")),
        check_vma=False,
    )
```

```python
import functools

import jax
import jax.numpy as jnp
from jax import lax
from jax.experimental import pallas as pl
from jax.experimental.pallas import tpu as pltpu
from jax.sharding import PartitionSpec as P

PANEL = 256
PIVOT_ITERS = 6
STEPS_A = 2
STEPS_B = 16

EXACT = lax.Precision.HIGHEST
SPLIT = lax.Precision.HIGH

def dot(x, y, precision):
    return jnp.dot(x, y, precision=precision, preferred_element_type=jnp.float32)


def pivot_inverse(pivot, precision):
    order = pivot.shape[0]
    down = lax.broadcasted_iota(jnp.int32, (order, order), 0)
    across = lax.broadcasted_iota(jnp.int32, (order, order), 1)
    eye = (down == across).astype(jnp.float32)
    kept = pivot * eye
    tall = 1.0 / jnp.sqrt(jnp.sum(kept, axis=1, keepdims=True))
    wide = 1.0 / jnp.sqrt(jnp.sum(kept, axis=0, keepdims=True))
    unit = pivot * tall * wide
    ceiling = jnp.max(jnp.sum(jnp.abs(unit), axis=1, keepdims=True), axis=0, keepdims=True)
    power = eye - unit / ceiling
    total = eye + power
    power = dot(power, power, precision)
    for turn in range(1, PIVOT_ITERS - 1):
        both = dot(power, jnp.concatenate([power, total], 1), precision)
        total = total + both[:, order:]
        power = both[:, :order]
    total = total + dot(power, total, precision)
    return total / ceiling * tall * wide


class Plan:
    def __init__(self, mesh):
        self.rows = mesh.shape["row"]
        self.cols = mesh.shape["col"]
        line = list(mesh.devices.reshape(self.rows, self.cols)[0])
        at = [tuple(getattr(device, "coords", (place, 0, 0))) for place, device in enumerate(line)]
        paired = self.cols % 2 == 0 and all(at[2 * i] == at[2 * i + 1] for i in range(self.cols // 2))
        self.cores = 2 if paired else 1
        chips = at[:: self.cores]
        wide = len({chip[0] for chip in chips})
        tall = len({chip[1] for chip in chips})
        low_x, low_y = min(chip[0] for chip in chips), min(chip[1] for chip in chips)
        plane = [(x + low_x, y + low_y) for y in range(tall) for x in range(wide)]
        if [(chip[0], chip[1]) for chip in chips] != plane:
            wide, tall = len(chips), 1
        self.wide, self.tall = wide, tall


SLOTS = 4
WAYS = ((1, 0), (-1, 0), (0, 1), (0, -1))


def unit():
    down = lax.broadcasted_iota(jnp.int32, (PANEL, PANEL), 0)
    across = lax.broadcasted_iota(jnp.int32, (PANEL, PANEL), 1)
    return (down == across).astype(jnp.float32)


def squares(m):
    total = jnp.zeros((8, 128), jnp.float32)
    for j in range(m.shape[0]):
        value = m[j]
        folded = jnp.sum((value * value).reshape(-1, 8, PANEL), axis=0)
        total = total + folded[:, :128] + folded[:, 128:]
    return total


def sweep_kernel(
    plan, steps, wide_a, pieces,
    b_ref, a_ref, c_ref,
    o_ref, sums_ref, ar_ref, cr_ref, ac_ref, ad_ref,
    m, w, r, x, t, in_row, in_col,
    in_sem, row_recv, row_up, row_down, w_recv, w_send, w_pair,
    z_recv, z_send, ac_recv, ac_send, ac_pair, ad_recv, ad_send, ad_pair,
    sum_row_recv, sum_row_send, sum_col_recv, sum_col_send,
):
    tiles, height, _ = m.shape
    blocks = height // PANEL
    half = PANEL // 2
    me_row = lax.axis_index("row")
    me_col = lax.axis_index("col")
    cores = plan.cores
    chip = me_col // cores
    core = me_col % cores
    pair = chip * cores + (cores - 1 - core)
    at_x, at_y = chip % plan.wide, chip // plan.wide

    def to_row(place):
        return {"row": place, "col": me_col}

    def to_col(place):
        return {"row": me_row, "col": place}

    def remote(src, dst, send, recv, target):
        return pltpu.make_async_remote_copy(
            src_ref=src, dst_ref=dst, send_sem=send, recv_sem=recv,
            device_id=target, device_id_type=pl.DeviceIdType.MESH,
        )

    loads = [
        pltpu.make_async_copy(b_ref.at[:, pl.ds(j * PANEL, PANEL)], m.at[j], in_sem.at[j]) for j in range(tiles)
    ]
    for load in loads:
        load.start()

    barrier = pltpu.get_barrier_semaphore()
    for d in range(1, plan.rows):
        pl.semaphore_signal(
            barrier, inc=1, device_id=to_row((me_row + d) % plan.rows), device_id_type=pl.DeviceIdType.MESH
        )
    for d in range(1, plan.cols):
        pl.semaphore_signal(
            barrier, inc=1, device_id=to_col((me_col + d) % plan.cols), device_id_type=pl.DeviceIdType.MESH
        )
    pl.semaphore_wait(barrier, plan.rows + plan.cols - 2)
    for load in loads:
        load.wait()

    def row_root(p):
        return p // blocks

    def col_root(p):
        return p // tiles

    def row_copy(p, i, up):
        part = r.at[p, (p + i) % tiles]
        sem = (row_up if up else row_down).at[p, i]
        return remote(part, part, sem, row_recv.at[p, i], to_row(me_row + 1 if up else me_row - 1))

    def row_sends(p, i, act):
        @pl.when((me_row >= row_root(p)) & (me_row < plan.rows - 1))
        def _():
            act(row_copy(p, i, True))

        @pl.when((me_row <= row_root(p)) & (me_row > 0))
        def _():
            act(row_copy(p, i, False))

    def routes(root, h):
        at = root // cores
        from_x, from_y = at % plan.wide, at // plan.wide
        carry = me_col == root
        if cores == 2:
            carry = carry | ((chip != at) & (core == h))
        else:
            carry = carry | (me_col != root)
        found = []
        for way, (dx, dy) in enumerate(WAYS):
            span, place, origin = (plan.wide, at_x, from_x) if dx else (plan.tall, at_y, from_y)
            if span == 1:
                continue
            on = (place >= origin) & (place < span - 1) if dx + dy > 0 else (place <= origin) & (place > 0)
            if dx and h == 0:
                on = on & (at_y == from_y)
            if dy and h == 1:
                on = on & (at_x == from_x)
            target = (chip + dx + dy * plan.wide) * cores + (h if cores == 2 else 0)
            found.append((way, carry & on, target))
        return carry, found

    def panel_sends(root, h, ref, recv, send, couple, act):
        carry, found = routes(root, h)
        for way, on, target in found:

            @pl.when(on)
            def _():
                act(remote(ref, ref, send(way), recv, to_col(target)))

        if cores == 2:

            @pl.when(carry)
            def _():
                act(remote(ref, ref, couple, recv, to_col(pair)))

    def piece(p, h, i):
        start = ((p + 1 + i) % blocks) * PANEL + h * half
        return w.at[p, pl.ds(pl.multiple_of(start, half), half)]

    def w_sends(p, h, i, act):
        slot = p % SLOTS
        panel_sends(
            col_root(p), h, piece(p, h, i), w_recv.at[p, h, i],
            lambda way: w_send.at[way, slot, h, i], w_pair.at[slot, h, i], act,
        )

    def w_wait(p, h, i):
        remote(piece(p, h, i), piece(p, h, i), w_pair.at[0, 0, 0], w_recv.at[p, h, i], to_col(pair)).wait_recv()

    def start(copy):
        copy.start()

    def sent(copy):
        copy.wait_send()

    def take_carried(p, which):
        @pl.when(me_col != col_root(p))
        def _():
            for i in which:
                for h in range(2):
                    if cores == 2:

                        @pl.when((core == h) & (chip != col_root(p) // cores))
                        def _():
                            w_wait(p, h, i)
                            w_sends(p, h, i, start)

                    else:
                        w_wait(p, h, i)
                        w_sends(p, h, i, start)

    def take_other(p, which):
        if cores == 2:

            @pl.when(me_col != col_root(p))
            def _():
                home = chip == col_root(p) // cores
                for i in which:
                    for h in range(2):

                        @pl.when((core != h) | home)
                        def _():
                            w_wait(p, h, i)

    def drain(p):
        for i in range(blocks):
            for h in range(2):
                w_sends(p, h, i, sent)

    def block(p):
        return pl.ds(pl.multiple_of((p % blocks) * PANEL, PANEL), PANEL)

    def make_rows(p):
        for j in range(tiles):
            fresh = m[j, block(p), :]

            @pl.when(p == 0)
            def _():
                r[p, j] = fresh

            @pl.when(p > 0)
            def _():
                q = jnp.maximum(p - 1, 0)
                step = w[q, block(p), :]
                swept = (me_col == col_root(q)) & (q % tiles == j)

                @pl.when(swept)
                def _():
                    r[p, j] = -step

                @pl.when(jnp.logical_not(swept))
                def _():
                    r[p, j] = fresh - dot(step, r[q, j], SPLIT)

    def make_w(p):
        j = p % tiles

        @pl.when(p == 0)
        def _():
            t[...] = m[j]

        @pl.when(p > 0)
        def _():
            q = jnp.maximum(p - 1, 0)
            t[...] = m[j] - dot(w[q], r[q, j], SPLIT)

        @pl.when(me_row == row_root(p))
        def _():
            t[block(p), :] = t[block(p), :] - unit()

        w[p] = dot(t[...], x[...], SPLIT)

    def update(q):
        for j in range(tiles):
            swept = (me_col == col_root(q)) & (q % tiles == j)

            @pl.when(swept)
            def _():
                m[j] = -w[q]

                @pl.when(me_row == row_root(q))
                def _():
                    m[j, block(q), :] = unit() - w[q, block(q), :]

            @pl.when(jnp.logical_not(swept))
            def _():
                m[j] = m[j] - dot(w[q], r[q, j], SPLIT)

    def z_copy(i, own):
        kind, low, high = pieces[i]
        there = (ar_ref if kind == "a" else cr_ref).at[:, pl.ds(low, high - low)]
        here = (a_ref if kind == "a" else c_ref).at[pl.ds(0, wide_a), pl.ds(low, high - low)] if own else there
        return remote(here, there, z_send.at[i], z_recv.at[i], to_row(jnp.minimum(me_row + 1, plan.rows - 1)))

    def z_turn(p):
        for i in range(len(pieces)):

            @pl.when((p == blocks * (me_row + 1) - 1 + i) & (me_row < plan.rows - 1))
            def _():
                @pl.when(me_row == 0)
                def _():
                    z_copy(i, True).start()

                @pl.when(me_row > 0)
                def _():
                    z_copy(i, False).wait_recv()
                    z_copy(i, False).start()

    def spread_turn(p, first, stride, here, there, recv, send, couple):
        rows = there.shape[0] // 2

        def half_of(ref, h):
            return ref.at[pl.ds(h * rows, rows)]

        def sends(ref, h, act):
            carry, found = routes(jnp.int32(0), h)
            for way, on, target in found:

                @pl.when(on)
                def _():
                    act(remote(half_of(ref, h), half_of(there, h), send.at[way, h], recv.at[h], to_col(target)))

            if cores == 2:

                @pl.when(carry)
                def _():
                    act(remote(half_of(ref, h), half_of(there, h), couple.at[h], recv.at[h], to_col(pair)))

        def wait(h):
            remote(half_of(there, h), half_of(there, h), couple.at[h], recv.at[h], to_col(pair)).wait_recv()

        turn = jnp.minimum(first + stride * (at_x + at_y), steps)

        @pl.when((p == turn) & (me_col == 0))
        def _():
            here(lambda ref: [sends(ref, h, start) for h in range(2)])

        @pl.when((p == turn) & (me_col != 0))
        def _():
            for h in range(2):
                if cores == 2:

                    @pl.when((core == h) & (chip != 0))
                    def _():
                        wait(h)
                        sends(there, h, start)

                else:
                    wait(h)
                    sends(there, h, start)

        def last():
            if cores == 2:

                @pl.when(me_col != 0)
                def _():
                    for h in range(2):

                        @pl.when((core != h) | (chip == 0))
                        def _():
                            wait(h)

            for h in range(2):
                sends(there, h, sent)

        return last

    def own_columns(act):
        act(a_ref.at[:, pl.ds(0, wide_a)])

    def own_top(act):
        @pl.when(me_row == 0)
        def _():
            act(a_ref.at[pl.ds(0, wide_a), pl.ds(0, wide_a)])

        @pl.when(me_row > 0)
        def _():
            act(ar_ref.at[:, pl.ds(0, wide_a)])

    def wait_top(p):
        @pl.when((p == steps - 2) & (me_row == plan.rows - 1) & (me_row > 0))
        def _():
            z_copy(0, False).wait_recv()

    def spread_turns(p):
        one = spread_turn(p, blocks, blocks, own_columns, ac_ref, ac_recv, ac_send, ac_pair)
        wait_top(p)
        two = spread_turn(p, steps - 2, 1, own_top, ad_ref, ad_recv, ad_send, ad_pair)
        return one, two

    b_part = squares(m)

    def step(p, carry):
        root = me_row == row_root(p)
        owner = me_col == col_root(p)
        q = jnp.maximum(p - 1, 0)

        @pl.when(p >= SLOTS)
        def _():
            drain(jnp.maximum(p - SLOTS, 0))

        @pl.when(jnp.logical_not(root))
        def _():
            row_copy(p, 0, True).wait_recv()
            row_sends(p, 0, start)

        @pl.when(root)
        def _():
            @pl.when(p > 0)
            def _():
                take_carried(q, range(1))
                take_other(q, range(1))

            make_rows(p)
            for i in range(tiles):
                row_sends(p, i, start)

        @pl.when(owner)
        def _():
            x[...] = pivot_inverse(r[p, p % tiles], SPLIT)

        @pl.when(p > 0)
        def _():
            @pl.when(jnp.logical_not(root))
            def _():
                take_carried(q, range(1))
                take_other(q, range(1))

            take_carried(q, range(1, blocks))
            take_other(q, range(1, blocks))

        @pl.when(owner)
        def _():
            make_w(p)
            for i in range(blocks):
                for h in range(2):
                    w_sends(p, h, i, start)

        @pl.when(jnp.logical_not(root))
        def _():
            for i in range(1, tiles):
                row_copy(p, i, True).wait_recv()
                row_sends(p, i, start)

        @pl.when(p > 0)
        def _():
            update(q)

        if WITH_A:
            z_turn(p)
            spread_turns(p)
        return carry

    lax.fori_loop(0, steps, step, 0)
    take_carried(steps - 1, range(blocks))
    take_other(steps - 1, range(blocks))
    update(steps - 1)

    stores = [
        pltpu.make_async_copy(m.at[j], o_ref.at[:, pl.ds(j * PANEL, PANEL)], in_sem.at[j]) for j in range(tiles)
    ]
    for store in stores:
        store.start()

    in_row[me_row, 0] = b_part
    in_row[me_row, 1] = squares(m)
    for d in range(1, plan.rows):
        place = in_row.at[me_row]
        remote(place, place, sum_row_send.at[d], sum_row_recv.at[d], to_row((me_row + d) % plan.rows)).start()
    if WITH_A:
        last = spread_turns(jnp.int32(steps))
    for d in range(1, plan.rows):
        place = in_row.at[(me_row + plan.rows - d) % plan.rows]
        remote(place, place, sum_row_send.at[d], sum_row_recv.at[d], to_row((me_row + d) % plan.rows)).wait_recv()
    in_col[me_col] = jnp.sum(in_row[...], axis=0)
    for d in range(1, plan.cols):
        place = in_col.at[me_col]
        remote(place, place, sum_col_send.at[d], sum_col_recv.at[d], to_col((me_col + d) % plan.cols)).start()
    for d in range(1, plan.cols):
        place = in_col.at[(me_col + plan.cols - d) % plan.cols]
        remote(place, place, sum_col_send.at[d], sum_col_recv.at[d], to_col((me_col + d) % plan.cols)).wait_recv()
    sums_ref[...] = jnp.sum(in_col[...], axis=0)

    if WITH_A:
        for finish in last:
            finish()

        @pl.when(me_row < plan.rows - 1)
        def _():
            for i in range(len(pieces)):
                z_copy(i, False).wait_send()

        @pl.when((me_row == plan.rows - 1) & (me_row > 0))
        def _():
            for i in range(1, len(pieces)):
                z_copy(i, False).wait_recv()

    for d in range(1, plan.rows):
        place = in_row.at[me_row]
        remote(place, place, sum_row_send.at[d], sum_row_recv.at[d], to_row((me_row + d) % plan.rows)).wait_send()
    for d in range(1, plan.cols):
        place = in_col.at[me_col]
        remote(place, place, sum_col_send.at[d], sum_col_recv.at[d], to_col((me_col + d) % plan.cols)).wait_send()

    def row_drain(p, carry):
        for i in range(tiles):
            row_sends(p, i, sent)
        return carry

    lax.fori_loop(0, steps, row_drain, 0)
    lax.fori_loop(steps - SLOTS, steps, lambda p, carry: (drain(p), carry)[1], 0)
    for store in stores:
        store.wait()


WITH_A = True


def sweep_b(plan, matrix, a_matrix, c_matrix):
    height, width = matrix.shape
    tiles = width // PANEL
    blocks = height // PANEL
    steps = STEPS_B
    wide_a = STEPS_A * PANEL
    a_cols, c_cols = a_matrix.shape[1], c_matrix.shape[1]
    pieces = [("a", 0, wide_a)]
    if a_cols > wide_a:
        pieces.append(("a", wide_a, a_cols))
    pieces.append(("c", 0, c_cols))
    assert blocks * (plan.rows - 1) + len(pieces) - 2 < steps
    assert wide_a <= min(a_matrix.shape)
    dma = pltpu.SemaphoreType.DMA
    vmem = pltpu.VMEM
    return pl.pallas_call(
        functools.partial(sweep_kernel, plan, steps, wide_a, pieces),
        out_shape=[
            jax.ShapeDtypeStruct((height, width), jnp.float32),
            jax.ShapeDtypeStruct((2, 8, 128), jnp.float32),
            jax.ShapeDtypeStruct((wide_a, a_cols), jnp.float32),
            jax.ShapeDtypeStruct((wide_a, c_cols), jnp.float32),
            jax.ShapeDtypeStruct((a_matrix.shape[0], wide_a), jnp.float32),
            jax.ShapeDtypeStruct((wide_a, wide_a), jnp.float32),
        ],
        in_specs=[pl.BlockSpec(memory_space=pl.ANY)] * 3,
        out_specs=[
            pl.BlockSpec(memory_space=pl.ANY),
            pl.BlockSpec(memory_space=pltpu.VMEM),
        ]
        + [pl.BlockSpec(memory_space=pl.ANY)] * 4,
        scratch_shapes=[
            vmem((tiles, height, PANEL), jnp.float32),
            vmem((steps, height, PANEL), jnp.float32),
            vmem((steps, tiles, PANEL, PANEL), jnp.float32),
            vmem((PANEL, PANEL), jnp.float32),
            vmem((height, PANEL), jnp.float32),
            vmem((plan.rows, 2, 8, 128), jnp.float32),
            vmem((plan.cols, 2, 8, 128), jnp.float32),
            dma((tiles,)),
            dma((steps, tiles)),
            dma((steps, tiles)),
            dma((steps, tiles)),
            dma((steps, 2, blocks)),
            dma((4, SLOTS, 2, blocks)),
            dma((SLOTS, 2, blocks)),
            dma((len(pieces),)),
            dma((len(pieces),)),
            dma((2,)),
            dma((4, 2)),
            dma((2,)),
            dma((2,)),
            dma((4, 2)),
            dma((2,)),
            dma((plan.rows,)),
            dma((plan.rows,)),
            dma((plan.cols,)),
            dma((plan.cols,)),
        ],
        compiler_params=pltpu.CompilerParams(
            collective_id=0, has_side_effects=True, vmem_limit_bytes=56 * 1024 * 1024
        ),
        name="sweep_b",
    )(matrix, a_matrix, c_matrix)


def finish_kernel(
    wide_a, tile, a_any, c_any, ar_any, cr_any, ac_any, ad_any, a_blk, c_blk, ao_blk, co_blk,
    col, rows, top, w, sem,
):
    me_row = lax.axis_index("row")
    me_col = lax.axis_index("col")
    a_cols = a_blk.shape[1]
    count = wide_a // PANEL
    here = pl.program_id(0)

    def part(s):
        return pl.ds(s * PANEL, PANEL)

    @pl.when(here == 0)
    def _():
        top_row, left = me_row == 0, me_col == 0

        def fetch(on, src, dst, i):
            @pl.when(on)
            def _():
                pltpu.make_async_copy(src, dst, sem.at[i]).start()

        def fetched(dst, i):
            pltpu.make_async_copy(dst, dst, sem.at[i]).wait()

        first = pl.ds(0, wide_a)
        a_part = rows.at[:, pl.ds(0, a_cols)]
        c_part = rows.at[:, pl.ds(a_cols, rows.shape[1] - a_cols)]
        fetch(left & top_row, a_any.at[first, first], top, 0)
        fetch(left & jnp.logical_not(top_row), ar_any.at[:, first], top, 0)
        fetch(jnp.logical_not(left), ad_any, top, 0)
        fetch(left, a_any.at[:, first], col, 1)
        fetch(jnp.logical_not(left), ac_any, col, 1)
        fetch(top_row, a_any.at[first], a_part, 2)
        fetch(jnp.logical_not(top_row), ar_any, a_part, 2)
        fetch(top_row, c_any.at[first], c_part, 3)
        fetch(jnp.logical_not(top_row), cr_any, c_part, 3)
        for i, dst in enumerate((top, col, a_part, c_part)):
            fetched(dst, i)

        for s in range(count):
            inverse = pivot_inverse(top[part(s), part(s)], SPLIT)
            top[part(s), part(s)] = top[part(s), part(s)] - unit()

            @pl.when(top_row)
            def _():
                col[part(s), part(s)] = col[part(s), part(s)] - unit()

            w[:, part(s)] = dot(col[:, part(s)], inverse, SPLIT)

            @pl.when(left)
            def _():
                rows[:, part(s)] = jnp.zeros((wide_a, PANEL), jnp.float32)
                rows[part(s), part(s)] = unit()

            for later in range(s + 1, count):
                near = dot(top[part(later), part(s)], inverse, SPLIT)
                rows[part(later), :] = rows[part(later), :] - dot(near, rows[part(s), :], SPLIT)
                col[:, part(later)] = col[:, part(later)] - dot(w[:, part(s)], top[part(s), part(later)], SPLIT)
                for after in range(s + 1, count):
                    top[part(later), part(after)] = top[part(later), part(after)] - dot(
                        near, top[part(s), part(after)], SPLIT
                    )

    mine = pl.ds(pl.multiple_of(here * tile, tile), tile)
    taken = dot(w[mine, :], rows[...], SPLIT)
    ao_blk[...] = a_blk[...] - taken[:, :a_cols]
    co_blk[...] = c_blk[...] - taken[:, a_cols:]

    @pl.when(me_col == 0)
    def _():
        down = lax.broadcasted_iota(jnp.int32, (tile, wide_a), 0) + here * tile + me_row * a_any.shape[0]
        across = lax.broadcasted_iota(jnp.int32, (tile, wide_a), 1)
        ao_blk[:, :wide_a] = (down == across).astype(jnp.float32) - taken[:, :wide_a]


def finish_a(a_matrix, c_matrix, a_rows, c_rows, a_cols, a_top):
    height, width = a_matrix.shape
    c_width = c_matrix.shape[1]
    wide_a = a_cols.shape[1]
    tile = PANEL
    return pl.pallas_call(
        functools.partial(finish_kernel, wide_a, tile),
        grid=(height // tile,),
        out_shape=[
            jax.ShapeDtypeStruct((height, width), jnp.float32),
            jax.ShapeDtypeStruct((height, c_width), jnp.float32),
        ],
        in_specs=[pl.BlockSpec(memory_space=pl.ANY)] * 6
        + [pl.BlockSpec((tile, width), lambda i: (i, 0)), pl.BlockSpec((tile, c_width), lambda i: (i, 0))],
        out_specs=[pl.BlockSpec((tile, width), lambda i: (i, 0)), pl.BlockSpec((tile, c_width), lambda i: (i, 0))],
        scratch_shapes=[
            pltpu.VMEM((height, wide_a), jnp.float32),
            pltpu.VMEM((wide_a, width + c_width), jnp.float32),
            pltpu.VMEM((wide_a, wide_a), jnp.float32),
            pltpu.VMEM((height, wide_a), jnp.float32),
            pltpu.SemaphoreType.DMA((4,)),
        ],
        compiler_params=pltpu.CompilerParams(vmem_limit_bytes=48 * 1024 * 1024),
        name="finish_a",
    )(a_matrix, c_matrix, a_rows, c_rows, a_cols, a_top, a_matrix, c_matrix)


def body(plan, a_matrix, b_matrix, c_matrix):
    b_inverse, sums, a_rows, c_rows, a_cols, a_top = sweep_b(plan, b_matrix, a_matrix, c_matrix)
    a_swept, c_swept = finish_a(a_matrix, c_matrix, a_rows, c_rows, a_cols, a_top)
    b_squares, inv_squares = jnp.sum(sums[0]), jnp.sum(sums[1])
    scale = jnp.sqrt(jnp.sqrt(inv_squares / b_squares))
    b_next = 0.5 * (scale * b_matrix + b_inverse / scale)
    return (a_swept, c_swept, b_next)


def solution(mesh):
    return jax.shard_map(
        functools.partial(body, Plan(mesh)),
        mesh=mesh,
        in_specs=(P("row", "col"), P("row", "col"), P("row", "col")),
        out_specs=(P("row", "col"), P("row", "col"), P("row", "col")),
        check_vma=False,
    )
```

```python
import functools

import jax
import jax.numpy as jnp
from jax import lax
from jax.experimental import pallas as pl
from jax.experimental.pallas import tpu as pltpu
from jax.sharding import PartitionSpec as P

PANEL = 256
PIVOT_ITERS = 6
STEPS_A = 2
STEPS_B = 16

EXACT = lax.Precision.HIGHEST
SPLIT = lax.Precision.HIGH

def dot(x, y, precision):
    return jnp.dot(x, y, precision=precision, preferred_element_type=jnp.float32)


def pivot_inverse(pivot, precision):
    order = pivot.shape[0]
    down = lax.broadcasted_iota(jnp.int32, (order, order), 0)
    across = lax.broadcasted_iota(jnp.int32, (order, order), 1)
    eye = (down == across).astype(jnp.float32)
    kept = pivot * eye
    tall = 1.0 / jnp.sqrt(jnp.sum(kept, axis=1, keepdims=True))
    wide = 1.0 / jnp.sqrt(jnp.sum(kept, axis=0, keepdims=True))
    unit = pivot * tall * wide
    ceiling = jnp.max(jnp.sum(jnp.abs(unit), axis=1, keepdims=True), axis=0, keepdims=True)
    power = eye - unit / ceiling
    total = eye + power
    power = dot(power, power, precision)
    for turn in range(1, PIVOT_ITERS - 1):
        both = dot(power, jnp.concatenate([power, total], 1), precision)
        total = total + both[:, order:]
        power = both[:, :order]
    total = total + dot(power, total, precision)
    return total / ceiling * tall * wide


class Plan:
    def __init__(self, mesh):
        self.rows = mesh.shape["row"]
        self.cols = mesh.shape["col"]
        line = list(mesh.devices.reshape(self.rows, self.cols)[0])
        at = [tuple(getattr(device, "coords", (place, 0, 0))) for place, device in enumerate(line)]
        paired = self.cols % 2 == 0 and all(at[2 * i] == at[2 * i + 1] for i in range(self.cols // 2))
        self.cores = 2 if paired else 1
        chips = at[:: self.cores]
        wide = len({chip[0] for chip in chips})
        tall = len({chip[1] for chip in chips})
        low_x, low_y = min(chip[0] for chip in chips), min(chip[1] for chip in chips)
        plane = [(x + low_x, y + low_y) for y in range(tall) for x in range(wide)]
        if [(chip[0], chip[1]) for chip in chips] != plane:
            wide, tall = len(chips), 1
        self.wide, self.tall = wide, tall


SLOTS = 4
WAYS = ((1, 0), (-1, 0), (0, 1), (0, -1))


def unit():
    down = lax.broadcasted_iota(jnp.int32, (PANEL, PANEL), 0)
    across = lax.broadcasted_iota(jnp.int32, (PANEL, PANEL), 1)
    return (down == across).astype(jnp.float32)


def squares(m):
    total = jnp.zeros((8, 128), jnp.float32)
    for j in range(m.shape[0]):
        value = m[j]
        folded = jnp.sum((value * value).reshape(-1, 8, PANEL), axis=0)
        total = total + folded[:, :128] + folded[:, 128:]
    return total


def sweep_kernel(
    plan, steps, wide_a, pieces,
    b_ref, a_ref, c_ref,
    o_ref, sums_ref, ar_ref, cr_ref, ac_ref,
    m, w, r, x, t, in_row, in_col,
    in_sem, row_recv, row_up, row_down, w_recv, w_send, w_pair,
    z_recv, z_send, ac_recv, ac_send, ac_pair,
    sum_row_recv, sum_row_send, sum_col_recv, sum_col_send,
):
    tiles, height, _ = m.shape
    blocks = height // PANEL
    square = plan.wide == 2 and plan.tall == 2
    kinds = ("xy", "yx")
    me_row = lax.axis_index("row")
    me_col = lax.axis_index("col")
    cores = plan.cores
    chip = me_col // cores
    core = me_col % cores
    pair = chip * cores + (cores - 1 - core)
    at_x, at_y = chip % plan.wide, chip // plan.wide

    def to_row(place):
        return {"row": place, "col": me_col}

    def to_col(place):
        return {"row": me_row, "col": place}

    def remote(src, dst, send, recv, target):
        return pltpu.make_async_remote_copy(
            src_ref=src, dst_ref=dst, send_sem=send, recv_sem=recv,
            device_id=target, device_id_type=pl.DeviceIdType.MESH,
        )

    loads = [
        pltpu.make_async_copy(b_ref.at[:, pl.ds(j * PANEL, PANEL)], m.at[j], in_sem.at[j]) for j in range(tiles)
    ]
    for load in loads:
        load.start()

    barrier = pltpu.get_barrier_semaphore()
    for d in range(1, plan.rows):
        pl.semaphore_signal(
            barrier, inc=1, device_id=to_row((me_row + d) % plan.rows), device_id_type=pl.DeviceIdType.MESH
        )
    for d in range(1, plan.cols):
        pl.semaphore_signal(
            barrier, inc=1, device_id=to_col((me_col + d) % plan.cols), device_id_type=pl.DeviceIdType.MESH
        )
    pl.semaphore_wait(barrier, plan.rows + plan.cols - 2)
    for load in loads:
        load.wait()

    def row_root(p):
        return p // blocks

    def col_root(p):
        return p // tiles

    def row_copy(p, i, up):
        part = r.at[p, (p + i) % tiles]
        sem = (row_up if up else row_down).at[p, i]
        return remote(part, part, sem, row_recv.at[p, i], to_row(me_row + 1 if up else me_row - 1))

    def row_sends(p, i, act):
        @pl.when((me_row >= row_root(p)) & (me_row < plan.rows - 1))
        def _():
            act(row_copy(p, i, True))

        @pl.when((me_row <= row_root(p)) & (me_row > 0))
        def _():
            act(row_copy(p, i, False))

    def routes(root, kind, h):
        at = root // cores
        from_x, from_y = at % plan.wide, at // plan.wide
        carry = me_col == root
        if cores == 2:
            carry = carry | ((chip != at) & (core == h))
        else:
            carry = carry | (me_col != root)
        aside, apart = at_x != from_x, at_y != from_y
        found = []
        for way, (dx, dy) in enumerate(WAYS):
            span, place, origin = (plan.wide, at_x, from_x) if dx else (plan.tall, at_y, from_y)
            if span == 1:
                continue
            if kind in ("xy", "yx"):
                on = (place >= origin) & (place < span - 1) if dx + dy > 0 else (place <= origin) & (place > 0)
                if dx and kind == "xy":
                    on = on & jnp.logical_not(apart)
                if dy and kind == "yx":
                    on = on & jnp.logical_not(aside)
            else:
                on = place < span - 1 if dx + dy > 0 else place > 0
                same = aside == apart
                if kind == "ring x":
                    on = on & (same if dx else aside & jnp.logical_not(apart))
                else:
                    on = on & (same if dy else apart & jnp.logical_not(aside))
            target = (chip + dx + dy * plan.wide) * cores + (h if cores == 2 else 0)
            found.append((way, carry & on, target))
        return carry, found

    def panel_sends(root, kind, h, src, dst, recv, send, couple, act, ways=(0, 1, 2, 3), across=True):
        carry, found = routes(root, kind, h)
        for way, on, target in found:
            if way not in ways:
                continue

            @pl.when(on)
            def _():
                act(remote(src, dst, send(way), recv, to_col(target)))

        if cores == 2 and across:

            @pl.when(carry)
            def _():
                act(remote(src, dst, couple, recv, to_col(pair)))

    def piece(p, i):
        return w.at[p, pl.ds(pl.multiple_of(((p + 1 + i) % blocks) * PANEL, PANEL), PANEL)]

    def w_sends(p, i, act, **which):
        slot = p % SLOTS
        part = piece(p, i)
        panel_sends(
            col_root(p), kinds[i % len(kinds)], i % 2, part, part, w_recv.at[p, i],
            lambda way: w_send.at[way, slot, i], w_pair.at[slot, i], act, **which,
        )

    def w_wait(p, i):
        remote(piece(p, i), piece(p, i), w_pair.at[0, 0], w_recv.at[p, i], to_col(pair)).wait_recv()

    def start(copy):
        copy.start()

    def sent(copy):
        copy.wait_send()

    def take(p, which):
        @pl.when(me_col != col_root(p))
        def _():
            home = chip == col_root(p) // cores
            if cores == 1:
                for i in which:
                    w_wait(p, i)
                    w_sends(p, i, start)
                return
            for h in range(2):

                @pl.when(jnp.logical_not(home) & (core == h))
                def _():
                    for i in which:
                        if i % 2 == h:
                            w_wait(p, i)
                            w_sends(p, i, start)
                    for i in which:
                        if i % 2 != h:
                            w_wait(p, i)

            @pl.when(home)
            def _():
                for i in which:
                    w_wait(p, i)

    def drain(p):
        for i in range(blocks):
            w_sends(p, i, sent)

    def block(p):
        return pl.ds(pl.multiple_of((p % blocks) * PANEL, PANEL), PANEL)

    def make_rows(p):
        for j in range(tiles):
            fresh = m[j, block(p), :]

            @pl.when(p == 0)
            def _():
                r[p, j] = fresh

            @pl.when(p > 0)
            def _():
                q = jnp.maximum(p - 1, 0)
                step = w[q, block(p), :]
                swept = (me_col == col_root(q)) & (q % tiles == j)

                @pl.when(swept)
                def _():
                    r[p, j] = -step

                @pl.when(jnp.logical_not(swept))
                def _():
                    r[p, j] = fresh - dot(step, r[q, j], SPLIT)

    def make_w(p):
        j = p % tiles

        @pl.when(p == 0)
        def _():
            t[...] = m[j]

        @pl.when(p > 0)
        def _():
            q = jnp.maximum(p - 1, 0)
            t[...] = m[j] - dot(w[q], r[q, j], SPLIT)

        @pl.when(me_row == row_root(p))
        def _():
            t[block(p), :] = t[block(p), :] - unit()

        w[p] = dot(t[...], x[...], SPLIT)

    def update(q):
        for j in range(tiles):
            swept = (me_col == col_root(q)) & (q % tiles == j)

            @pl.when(swept)
            def _():
                m[j] = -w[q]

                @pl.when(me_row == row_root(q))
                def _():
                    m[j, block(q), :] = unit() - w[q, block(q), :]

            @pl.when(jnp.logical_not(swept))
            def _():
                m[j] = m[j] - dot(w[q], r[q, j], SPLIT)

    def z_copy(i, own):
        kind, low, high = pieces[i]
        there = (ar_ref if kind == "a" else cr_ref).at[:, pl.ds(low, high - low)]
        here = (a_ref if kind == "a" else c_ref).at[pl.ds(0, wide_a), pl.ds(low, high - low)] if own else there
        return remote(here, there, z_send.at[i], z_recv.at[i], to_row(jnp.minimum(me_row + 1, plan.rows - 1)))

    def z_turn(p):
        for i in range(len(pieces)):

            @pl.when((p == blocks * (me_row + 1) - 1 + i) & (me_row < plan.rows - 1))
            def _():
                @pl.when(me_row == 0)
                def _():
                    z_copy(i, True).start()

                @pl.when(me_row > 0)
                def _():
                    z_copy(i, False).wait_recv()
                    z_copy(i, False).start()

    half = PANEL // 2
    top_parts = wide_a // PANEL
    top_turn = steps - 1 - top_parts
    tall_half = a_ref.shape[0] // 2
    first = pl.ds(0, wide_a)

    def a_there(c, h):
        if isinstance(c, int) and c == 0:
            return ac_ref.at[pl.ds(h * tall_half, tall_half)]
        return ac_ref.at[pl.ds(pl.multiple_of(2 * tall_half + (c - 1) * PANEL + h * half, half), half)]

    def a_own(c, h, act):
        if isinstance(c, int) and c == 0:
            act(a_ref.at[pl.ds(h * tall_half, tall_half), first])
            return
        spot = pl.ds(pl.multiple_of((c - 1) * PANEL + h * half, half), half)

        @pl.when(me_row == 0)
        def _():
            act(a_ref.at[spot, first])

        @pl.when(me_row > 0)
        def _():
            act(ar_ref.at[spot, first])

    def a_sends(c, h, src, act, **which):
        kind = "xy" if isinstance(c, int) and c == 0 else ("xy", "yx")[h]
        panel_sends(
            jnp.int32(0), kind, h, src, a_there(c, h), ac_recv.at[c, h],
            lambda way: ac_send.at[way, c, h], ac_pair.at[c, h], act, **which,
        )

    def a_wait(c, h):
        part = a_there(c, h)
        remote(part, part, ac_pair.at[c, h], ac_recv.at[c, h], to_col(pair)).wait_recv()

    def a_carries(h):
        return (chip != 0) & ((core == h) | (cores == 1))

    def a_pass(c, h):
        @pl.when(me_col == 0)
        def _():
            a_own(c, h, lambda ref: a_sends(c, h, ref, start))

        @pl.when(a_carries(h))
        def _():
            a_wait(c, h)
            a_sends(c, h, a_there(c, h), start)

    col_turn = jnp.where(
        at_y == 0, 2 * blocks + 2 * (at_x - 1), 3 * blocks + 2 * at_x + 2 * (at_y - 1)
    )

    def col_start(p):
        for h in range(2):

            @pl.when((me_col == 0) & (p == blocks))
            def _():
                a_own(0, h, lambda ref: a_sends(0, h, ref, start, ways=(0, 1)))

            @pl.when((me_col == 0) & (p == 2 * blocks))
            def _():
                a_own(0, h, lambda ref: a_sends(0, h, ref, start, ways=(2, 3), across=False))

    def col_pass(on):
        for h in range(2):

            @pl.when(a_carries(h) & on)
            def _():
                a_wait(0, h)
                a_sends(0, h, a_there(0, h), start)

    def wait_top():
        @pl.when((me_row == plan.rows - 1) & (me_row > 0))
        def _():
            z_copy(0, False).wait_recv()

    def a_turn(p):
        col_start(p)
        col_pass(p == col_turn)

        @pl.when(p == top_turn)
        def _():
            wait_top()

        for h in range(2):
            c = p - top_turn - at_x - at_y

            @pl.when((c >= 0) & (c < top_parts))
            def _():
                a_pass(1 + jnp.clip(c, 0, top_parts - 1), h)

    def a_last():
        col_pass(col_turn >= steps)
        for c in range(top_parts):
            for h in range(2):

                @pl.when(top_turn + c + at_x + at_y >= steps)
                def _():
                    a_pass(1 + c, h)

        if cores == 2:
            for h in range(2):

                @pl.when((me_col != 0) & ((core != h) | (chip == 0)))
                def _():
                    for c in range(1 + top_parts):
                        a_wait(c, h)

        for c in range(1 + top_parts):
            for h in range(2):
                a_sends(c, h, a_there(c, h), sent)

    b_part = squares(m)

    def step(p, carry):
        root = me_row == row_root(p)
        owner = me_col == col_root(p)
        q = jnp.maximum(p - 1, 0)

        @pl.when(p >= SLOTS)
        def _():
            drain(jnp.maximum(p - SLOTS, 0))

        early = blocks

        @pl.when(jnp.logical_not(root))
        def _():
            @pl.when(p > 0)
            def _():
                take(q, range(early))

            row_copy(p, 0, True).wait_recv()
            row_sends(p, 0, start)

        @pl.when(root)
        def _():
            @pl.when(p > 0)
            def _():
                take(q, range(1))

            make_rows(p)
            for i in range(tiles):
                row_sends(p, i, start)

        @pl.when(owner)
        def _():
            x[...] = pivot_inverse(r[p, p % tiles], SPLIT)

        @pl.when(p > 0)
        def _():
            @pl.when(root)
            def _():
                take(q, range(1, early))

            take(q, range(early, blocks))

        @pl.when(owner)
        def _():
            make_w(p)
            for i in range(blocks):
                w_sends(p, i, start, ways=())
            for i in range(blocks):
                w_sends(p, i, start, across=False)

        @pl.when(jnp.logical_not(root))
        def _():
            for i in range(1, tiles):
                row_copy(p, i, True).wait_recv()
                row_sends(p, i, start)

        @pl.when(p > 0)
        def _():
            update(q)

        if WITH_A:
            z_turn(p)
            a_turn(p)
        return carry

    lax.fori_loop(0, steps, step, 0)
    take(steps - 1, range(blocks))
    update(steps - 1)

    stores = [
        pltpu.make_async_copy(m.at[j], o_ref.at[:, pl.ds(j * PANEL, PANEL)], in_sem.at[j]) for j in range(tiles)
    ]
    for store in stores:
        store.start()

    in_row[me_row, 0] = b_part
    in_row[me_row, 1] = squares(m)
    for d in range(1, plan.rows):
        place = in_row.at[me_row]
        remote(place, place, sum_row_send.at[d], sum_row_recv.at[d], to_row((me_row + d) % plan.rows)).start()
    for d in range(1, plan.rows):
        place = in_row.at[(me_row + plan.rows - d) % plan.rows]
        remote(place, place, sum_row_send.at[d], sum_row_recv.at[d], to_row((me_row + d) % plan.rows)).wait_recv()
    in_col[me_col] = jnp.sum(in_row[...], axis=0)
    for d in range(1, plan.cols):
        place = in_col.at[me_col]
        remote(place, place, sum_col_send.at[d], sum_col_recv.at[d], to_col((me_col + d) % plan.cols)).start()
    for d in range(1, plan.cols):
        place = in_col.at[(me_col + plan.cols - d) % plan.cols]
        remote(place, place, sum_col_send.at[d], sum_col_recv.at[d], to_col((me_col + d) % plan.cols)).wait_recv()
    sums_ref[...] = jnp.sum(in_col[...], axis=0)

    if WITH_A:
        a_last()

        @pl.when(me_row < plan.rows - 1)
        def _():
            for i in range(len(pieces)):
                z_copy(i, False).wait_send()

        @pl.when((me_row == plan.rows - 1) & (me_row > 0))
        def _():
            for i in range(1, len(pieces)):
                z_copy(i, False).wait_recv()

    for d in range(1, plan.rows):
        place = in_row.at[me_row]
        remote(place, place, sum_row_send.at[d], sum_row_recv.at[d], to_row((me_row + d) % plan.rows)).wait_send()
    for d in range(1, plan.cols):
        place = in_col.at[me_col]
        remote(place, place, sum_col_send.at[d], sum_col_recv.at[d], to_col((me_col + d) % plan.cols)).wait_send()

    def row_drain(p, carry):
        for i in range(tiles):
            row_sends(p, i, sent)
        return carry

    lax.fori_loop(0, steps, row_drain, 0)
    lax.fori_loop(steps - SLOTS, steps, lambda p, carry: (drain(p), carry)[1], 0)
    for store in stores:
        store.wait()


WITH_A = True


def sweep_b(plan, matrix, a_matrix, c_matrix):
    height, width = matrix.shape
    tiles = width // PANEL
    blocks = height // PANEL
    steps = STEPS_B
    wide_a = STEPS_A * PANEL
    a_cols, c_cols = a_matrix.shape[1], c_matrix.shape[1]
    pieces = [("a", 0, wide_a)]
    if a_cols > wide_a:
        pieces.append(("a", wide_a, a_cols))
    pieces.append(("c", 0, c_cols))
    assert blocks * (plan.rows - 1) + len(pieces) - 2 < steps
    assert wide_a <= min(a_matrix.shape)
    dma = pltpu.SemaphoreType.DMA
    parts = 1 + wide_a // PANEL
    vmem = pltpu.VMEM
    return pl.pallas_call(
        functools.partial(sweep_kernel, plan, steps, wide_a, pieces),
        out_shape=[
            jax.ShapeDtypeStruct((height, width), jnp.float32),
            jax.ShapeDtypeStruct((2, 8, 128), jnp.float32),
            jax.ShapeDtypeStruct((wide_a, a_cols), jnp.float32),
            jax.ShapeDtypeStruct((wide_a, c_cols), jnp.float32),
            jax.ShapeDtypeStruct((a_matrix.shape[0] + wide_a, wide_a), jnp.float32),
        ],
        in_specs=[pl.BlockSpec(memory_space=pl.ANY)] * 3,
        out_specs=[
            pl.BlockSpec(memory_space=pl.ANY),
            pl.BlockSpec(memory_space=pltpu.VMEM),
        ]
        + [pl.BlockSpec(memory_space=pl.ANY)] * 3,
        scratch_shapes=[
            vmem((tiles, height, PANEL), jnp.float32),
            vmem((steps, height, PANEL), jnp.float32),
            vmem((steps, tiles, PANEL, PANEL), jnp.float32),
            vmem((PANEL, PANEL), jnp.float32),
            vmem((height, PANEL), jnp.float32),
            vmem((plan.rows, 2, 8, 128), jnp.float32),
            vmem((plan.cols, 2, 8, 128), jnp.float32),
            dma((tiles,)),
            dma((steps, tiles)),
            dma((steps, tiles)),
            dma((steps, tiles)),
            dma((steps, blocks)),
            dma((4, SLOTS, blocks)),
            dma((SLOTS, blocks)),
            dma((len(pieces),)),
            dma((len(pieces),)),
            dma((parts, 2)),
            dma((4, parts, 2)),
            dma((parts, 2)),
            dma((plan.rows,)),
            dma((plan.rows,)),
            dma((plan.cols,)),
            dma((plan.cols,)),
        ],
        compiler_params=pltpu.CompilerParams(
            collective_id=0, has_side_effects=True, vmem_limit_bytes=56 * 1024 * 1024
        ),
        name="sweep_b",
    )(matrix, a_matrix, c_matrix)


def halves(value):
    high = value.astype(jnp.bfloat16)
    return high, (value - high.astype(jnp.float32)).astype(jnp.bfloat16)


def finish_kernel(
    wide_a, tile, a_any, c_any, ar_any, cr_any, ac_any, a_blk, c_blk, ao_blk, co_blk,
    col, rows, top, w, rows3, w3, sem,
):
    me_row = lax.axis_index("row")
    me_col = lax.axis_index("col")
    a_cols = a_blk.shape[1]
    count = wide_a // PANEL
    here = pl.program_id(0)

    def part(s):
        return pl.ds(s * PANEL, PANEL)

    @pl.when(here == 0)
    def _():
        top_row, left = me_row == 0, me_col == 0

        def fetch(on, src, dst, i):
            @pl.when(on)
            def _():
                pltpu.make_async_copy(src, dst, sem.at[i]).start()

        def fetched(dst, i):
            pltpu.make_async_copy(dst, dst, sem.at[i]).wait()

        first = pl.ds(0, wide_a)
        a_part = rows.at[:, pl.ds(0, a_cols)]
        c_part = rows.at[:, pl.ds(a_cols, rows.shape[1] - a_cols)]
        fetch(left & top_row, a_any.at[first, first], top, 0)
        fetch(left & jnp.logical_not(top_row), ar_any.at[:, first], top, 0)
        fetch(jnp.logical_not(left), ac_any.at[pl.ds(a_any.shape[0], wide_a)], top, 0)
        fetch(left, a_any.at[:, first], col, 1)
        fetch(jnp.logical_not(left), ac_any.at[pl.ds(0, a_any.shape[0])], col, 1)
        fetch(top_row, a_any.at[first], a_part, 2)
        fetch(jnp.logical_not(top_row), ar_any, a_part, 2)
        fetch(top_row, c_any.at[first], c_part, 3)
        fetch(jnp.logical_not(top_row), cr_any, c_part, 3)
        for i, dst in enumerate((top, col, a_part, c_part)):
            fetched(dst, i)

        for s in range(count):
            inverse = pivot_inverse(top[part(s), part(s)], SPLIT)
            top[part(s), part(s)] = top[part(s), part(s)] - unit()

            @pl.when(top_row)
            def _():
                col[part(s), part(s)] = col[part(s), part(s)] - unit()

            w[:, part(s)] = dot(col[:, part(s)], inverse, SPLIT)

            @pl.when(left)
            def _():
                rows[:, part(s)] = jnp.zeros((wide_a, PANEL), jnp.float32)
                rows[part(s), part(s)] = unit()

            for later in range(s + 1, count):
                near = dot(top[part(later), part(s)], inverse, SPLIT)
                rows[part(later), :] = rows[part(later), :] - dot(near, rows[part(s), :], SPLIT)
                col[:, part(later)] = col[:, part(later)] - dot(w[:, part(s)], top[part(s), part(later)], SPLIT)
                for after in range(s + 1, count):
                    top[part(later), part(after)] = top[part(later), part(after)] - dot(
                        near, top[part(s), part(after)], SPLIT
                    )

        high, low = halves(rows[...])
        rows3[:wide_a], rows3[wide_a : 2 * wide_a], rows3[2 * wide_a :] = high, low, high
        high, low = halves(w[...])
        w3[:, :wide_a], w3[:, wide_a : 2 * wide_a], w3[:, 2 * wide_a :] = high, high, low

    mine = pl.ds(pl.multiple_of(here * tile, tile), tile)
    taken = jnp.dot(w3[mine, :], rows3[...], preferred_element_type=jnp.float32)
    ao_blk[...] = a_blk[...] - taken[:, :a_cols]
    co_blk[...] = c_blk[...] - taken[:, a_cols:]

    @pl.when(me_col == 0)
    def _():
        down = lax.broadcasted_iota(jnp.int32, (tile, wide_a), 0) + here * tile + me_row * a_any.shape[0]
        across = lax.broadcasted_iota(jnp.int32, (tile, wide_a), 1)
        ao_blk[:, :wide_a] = (down == across).astype(jnp.float32) - taken[:, :wide_a]


def finish_a(a_matrix, c_matrix, a_rows, c_rows, a_cols):
    height, width = a_matrix.shape
    c_width = c_matrix.shape[1]
    wide_a = a_cols.shape[1]
    tile = PANEL
    return pl.pallas_call(
        functools.partial(finish_kernel, wide_a, tile),
        grid=(height // tile,),
        out_shape=[
            jax.ShapeDtypeStruct((height, width), jnp.float32),
            jax.ShapeDtypeStruct((height, c_width), jnp.float32),
        ],
        in_specs=[pl.BlockSpec(memory_space=pl.ANY)] * 5
        + [pl.BlockSpec((tile, width), lambda i: (i, 0)), pl.BlockSpec((tile, c_width), lambda i: (i, 0))],
        out_specs=[pl.BlockSpec((tile, width), lambda i: (i, 0)), pl.BlockSpec((tile, c_width), lambda i: (i, 0))],
        scratch_shapes=[
            pltpu.VMEM((height, wide_a), jnp.float32),
            pltpu.VMEM((wide_a, width + c_width), jnp.float32),
            pltpu.VMEM((wide_a, wide_a), jnp.float32),
            pltpu.VMEM((height, wide_a), jnp.float32),
            pltpu.VMEM((3 * wide_a, width + c_width), jnp.bfloat16),
            pltpu.VMEM((height, 3 * wide_a), jnp.bfloat16),
            pltpu.SemaphoreType.DMA((4,)),
        ],
        compiler_params=pltpu.CompilerParams(vmem_limit_bytes=48 * 1024 * 1024),
        name="finish_a",
    )(a_matrix, c_matrix, a_rows, c_rows, a_cols, a_matrix, c_matrix)


def body(plan, a_matrix, b_matrix, c_matrix):
    b_inverse, sums, a_rows, c_rows, a_cols = sweep_b(plan, b_matrix, a_matrix, c_matrix)
    a_swept, c_swept = finish_a(a_matrix, c_matrix, a_rows, c_rows, a_cols)
    b_squares, inv_squares = jnp.sum(sums[0]), jnp.sum(sums[1])
    scale = jnp.sqrt(jnp.sqrt(inv_squares / b_squares))
    b_next = 0.5 * (scale * b_matrix + b_inverse / scale)
    return (a_swept, c_swept, b_next)


def solution(mesh):
    return jax.shard_map(
        functools.partial(body, Plan(mesh)),
        mesh=mesh,
        in_specs=(P("row", "col"), P("row", "col"), P("row", "col")),
        out_specs=(P("row", "col"), P("row", "col"), P("row", "col")),
        check_vma=False,
    )
```

```python
import functools

import jax
import jax.numpy as jnp
from jax import lax
from jax.experimental import pallas as pl
from jax.experimental.pallas import tpu as pltpu
from jax.sharding import PartitionSpec as P

PANEL = 256
PIVOT_ITERS = 6
STEPS_A = 2
STEPS_B = 16

EXACT = lax.Precision.HIGHEST
SPLIT = lax.Precision.HIGH

def dot(x, y, precision):
    return jnp.dot(x, y, precision=precision, preferred_element_type=jnp.float32)


def pivot_inverse(pivot, precision):
    order = pivot.shape[0]
    down = lax.broadcasted_iota(jnp.int32, (order, order), 0)
    across = lax.broadcasted_iota(jnp.int32, (order, order), 1)
    eye = (down == across).astype(jnp.float32)
    kept = pivot * eye
    tall = 1.0 / jnp.sqrt(jnp.sum(kept, axis=1, keepdims=True))
    wide = 1.0 / jnp.sqrt(jnp.sum(kept, axis=0, keepdims=True))
    unit = pivot * tall * wide
    ceiling = jnp.max(jnp.sum(jnp.abs(unit), axis=1, keepdims=True), axis=0, keepdims=True)
    power = eye - unit / ceiling
    total = eye + power
    power = dot(power, power, precision)
    for turn in range(1, PIVOT_ITERS - 1):
        both = dot(power, jnp.concatenate([power, total], 1), precision)
        total = total + both[:, order:]
        power = both[:, :order]
    total = total + dot(power, total, precision)
    return total / ceiling * tall * wide


class Plan:
    def __init__(self, mesh):
        self.rows = mesh.shape["row"]
        self.cols = mesh.shape["col"]
        line = list(mesh.devices.reshape(self.rows, self.cols)[0])
        at = [tuple(getattr(device, "coords", (place, 0, 0))) for place, device in enumerate(line)]
        paired = self.cols % 2 == 0 and all(at[2 * i] == at[2 * i + 1] for i in range(self.cols // 2))
        self.cores = 2 if paired else 1
        chips = at[:: self.cores]
        wide = len({chip[0] for chip in chips})
        tall = len({chip[1] for chip in chips})
        low_x, low_y = min(chip[0] for chip in chips), min(chip[1] for chip in chips)
        plane = [(x + low_x, y + low_y) for y in range(tall) for x in range(wide)]
        if [(chip[0], chip[1]) for chip in chips] != plane:
            wide, tall = len(chips), 1
        self.wide, self.tall = wide, tall


SLOTS = 4
WAYS = ((1, 0), (-1, 0), (0, 1), (0, -1))


def unit():
    down = lax.broadcasted_iota(jnp.int32, (PANEL, PANEL), 0)
    across = lax.broadcasted_iota(jnp.int32, (PANEL, PANEL), 1)
    return (down == across).astype(jnp.float32)


def squares(m):
    total = jnp.zeros((8, 128), jnp.float32)
    for j in range(m.shape[0]):
        value = m[j]
        folded = jnp.sum((value * value).reshape(-1, 8, PANEL), axis=0)
        total = total + folded[:, :128] + folded[:, 128:]
    return total


def sweep_kernel(
    plan, steps, wide_a, pieces,
    b_ref, a_ref, c_ref,
    o_ref, sums_ref, ar_ref, cr_ref, ac_ref,
    m, w, r, x, t, in_row, in_col,
    in_sem, row_recv, row_up, row_down, w_recv, w_send, w_pair,
    z_recv, z_send, ac_recv, ac_send, ac_pair,
    sum_row_recv, sum_row_send, sum_col_recv, sum_col_send,
):
    tiles, height, _ = m.shape
    blocks = height // PANEL
    square = plan.wide == 2 and plan.tall == 2
    kinds = ("xy", "yx")
    me_row = lax.axis_index("row")
    me_col = lax.axis_index("col")
    cores = plan.cores
    chip = me_col // cores
    core = me_col % cores
    pair = chip * cores + (cores - 1 - core)
    at_x, at_y = chip % plan.wide, chip // plan.wide

    def to_row(place):
        return {"row": place, "col": me_col}

    def to_col(place):
        return {"row": me_row, "col": place}

    def remote(src, dst, send, recv, target):
        return pltpu.make_async_remote_copy(
            src_ref=src, dst_ref=dst, send_sem=send, recv_sem=recv,
            device_id=target, device_id_type=pl.DeviceIdType.MESH,
        )

    loads = [
        pltpu.make_async_copy(b_ref.at[:, pl.ds(j * PANEL, PANEL)], m.at[j], in_sem.at[j]) for j in range(tiles)
    ]
    for load in loads:
        load.start()

    barrier = pltpu.get_barrier_semaphore()
    for d in range(1, plan.rows):
        pl.semaphore_signal(
            barrier, inc=1, device_id=to_row((me_row + d) % plan.rows), device_id_type=pl.DeviceIdType.MESH
        )
    for d in range(1, plan.cols):
        pl.semaphore_signal(
            barrier, inc=1, device_id=to_col((me_col + d) % plan.cols), device_id_type=pl.DeviceIdType.MESH
        )
    pl.semaphore_wait(barrier, plan.rows + plan.cols - 2)
    for load in loads:
        load.wait()

    def row_root(p):
        return p // blocks

    def col_root(p):
        return p // tiles

    def row_copy(p, i, up):
        part = r.at[p, (p + i) % tiles]
        sem = (row_up if up else row_down).at[p, i]
        return remote(part, part, sem, row_recv.at[p, i], to_row(me_row + 1 if up else me_row - 1))

    def row_sends(p, i, act):
        @pl.when((me_row >= row_root(p)) & (me_row < plan.rows - 1))
        def _():
            act(row_copy(p, i, True))

        @pl.when((me_row <= row_root(p)) & (me_row > 0))
        def _():
            act(row_copy(p, i, False))

    def routes(root, kind, h):
        at = root // cores
        from_x, from_y = at % plan.wide, at // plan.wide
        carry = me_col == root
        if cores == 2:
            carry = carry | ((chip != at) & (core == h))
        else:
            carry = carry | (me_col != root)
        aside, apart = at_x != from_x, at_y != from_y
        found = []
        for way, (dx, dy) in enumerate(WAYS):
            span, place, origin = (plan.wide, at_x, from_x) if dx else (plan.tall, at_y, from_y)
            if span == 1:
                continue
            if kind in ("xy", "yx"):
                on = (place >= origin) & (place < span - 1) if dx + dy > 0 else (place <= origin) & (place > 0)
                if dx and kind == "xy":
                    on = on & jnp.logical_not(apart)
                if dy and kind == "yx":
                    on = on & jnp.logical_not(aside)
            else:
                on = place < span - 1 if dx + dy > 0 else place > 0
                same = aside == apart
                if kind == "ring x":
                    on = on & (same if dx else aside & jnp.logical_not(apart))
                else:
                    on = on & (same if dy else apart & jnp.logical_not(aside))
            target = (chip + dx + dy * plan.wide) * cores + (h if cores == 2 else 0)
            found.append((way, carry & on, target))
        return carry, found

    def panel_sends(root, kind, h, src, dst, recv, send, couple, act, ways=(0, 1, 2, 3), across=True):
        carry, found = routes(root, kind, h)
        for way, on, target in found:
            if way not in ways:
                continue

            @pl.when(on)
            def _():
                act(remote(src, dst, send(way), recv, to_col(target)))

        if cores == 2 and across:

            @pl.when(carry)
            def _():
                act(remote(src, dst, couple, recv, to_col(pair)))

    def piece(p, i):
        return w.at[p, pl.ds(pl.multiple_of(((p + 1 + i) % blocks) * PANEL, PANEL), PANEL)]

    def w_sends(p, i, act, **which):
        slot = p % SLOTS
        part = piece(p, i)
        panel_sends(
            col_root(p), kinds[i % len(kinds)], i % 2, part, part, w_recv.at[p, i],
            lambda way: w_send.at[way, slot, i], w_pair.at[slot, i], act, **which,
        )

    def w_wait(p, i):
        remote(piece(p, i), piece(p, i), w_pair.at[0, 0], w_recv.at[p, i], to_col(pair)).wait_recv()

    def start(copy):
        copy.start()

    def sent(copy):
        copy.wait_send()

    def take(p, which):
        @pl.when(me_col != col_root(p))
        def _():
            home = chip == col_root(p) // cores
            if cores == 1:
                for i in which:
                    w_wait(p, i)
                    w_sends(p, i, start)
                return
            for h in range(2):

                @pl.when(jnp.logical_not(home) & (core == h))
                def _():
                    for i in which:
                        if i % 2 == h:
                            w_wait(p, i)
                            w_sends(p, i, start)
                    for i in which:
                        if i % 2 != h:
                            w_wait(p, i)

            @pl.when(home)
            def _():
                for i in which:
                    w_wait(p, i)

    def drain(p):
        for i in range(blocks):
            w_sends(p, i, sent)

    def block(p):
        return pl.ds(pl.multiple_of((p % blocks) * PANEL, PANEL), PANEL)

    def make_rows(p):
        for j in range(tiles):
            fresh = m[j, block(p), :]

            @pl.when(p == 0)
            def _():
                r[p, j] = fresh

            @pl.when(p > 0)
            def _():
                q = jnp.maximum(p - 1, 0)
                step = w[q, block(p), :]
                swept = (me_col == col_root(q)) & (q % tiles == j)

                @pl.when(swept)
                def _():
                    r[p, j] = -step

                @pl.when(jnp.logical_not(swept))
                def _():
                    r[p, j] = fresh - dot(step, r[q, j], SPLIT)

    def make_w(p):
        j = p % tiles

        @pl.when(p == 0)
        def _():
            t[...] = m[j]

        @pl.when(p > 0)
        def _():
            q = jnp.maximum(p - 1, 0)
            t[...] = m[j] - dot(w[q], r[q, j], SPLIT)

        @pl.when(me_row == row_root(p))
        def _():
            t[block(p), :] = t[block(p), :] - unit()

        w[p] = dot(t[...], x[...], SPLIT)

    def update(q):
        for j in range(tiles):
            swept = (me_col == col_root(q)) & (q % tiles == j)

            @pl.when(swept)
            def _():
                m[j] = -w[q]

                @pl.when(me_row == row_root(q))
                def _():
                    m[j, block(q), :] = unit() - w[q, block(q), :]

            @pl.when(jnp.logical_not(swept))
            def _():
                m[j] = m[j] - dot(w[q], r[q, j], SPLIT)

    def z_copy(i, own):
        kind, low, high = pieces[i]
        there = (ar_ref if kind == "a" else cr_ref).at[:, pl.ds(low, high - low)]
        here = (a_ref if kind == "a" else c_ref).at[pl.ds(0, wide_a), pl.ds(low, high - low)] if own else there
        return remote(here, there, z_send.at[i], z_recv.at[i], to_row(jnp.minimum(me_row + 1, plan.rows - 1)))

    def z_turn(p):
        for i in range(len(pieces)):

            @pl.when((p == blocks * (me_row + 1) - 1 + i) & (me_row < plan.rows - 1))
            def _():
                @pl.when(me_row == 0)
                def _():
                    z_copy(i, True).start()

                @pl.when(me_row > 0)
                def _():
                    z_copy(i, False).wait_recv()
                    z_copy(i, False).start()

    half = PANEL // 2
    top_parts = wide_a // PANEL
    top_turn = steps - 1 - top_parts
    tall_half = a_ref.shape[0] // 2
    first = pl.ds(0, wide_a)

    def a_there(c, h):
        if isinstance(c, int) and c == 0:
            return ac_ref.at[pl.ds(h * tall_half, tall_half)]
        return ac_ref.at[pl.ds(pl.multiple_of(2 * tall_half + (c - 1) * PANEL + h * half, half), half)]

    def a_own(c, h, act):
        if isinstance(c, int) and c == 0:
            act(a_ref.at[pl.ds(h * tall_half, tall_half), first])
            return
        spot = pl.ds(pl.multiple_of((c - 1) * PANEL + h * half, half), half)

        @pl.when(me_row == 0)
        def _():
            act(a_ref.at[spot, first])

        @pl.when(me_row > 0)
        def _():
            act(ar_ref.at[spot, first])

    def a_sends(c, h, src, act, **which):
        kind = "xy" if isinstance(c, int) and c == 0 else ("xy", "yx")[h]
        panel_sends(
            jnp.int32(0), kind, h, src, a_there(c, h), ac_recv.at[c, h],
            lambda way: ac_send.at[way, c, h], ac_pair.at[c, h], act, **which,
        )

    def a_wait(c, h):
        part = a_there(c, h)
        remote(part, part, ac_pair.at[c, h], ac_recv.at[c, h], to_col(pair)).wait_recv()

    def a_carries(h):
        return (chip != 0) & ((core == h) | (cores == 1))

    def a_pass(c, h):
        @pl.when(me_col == 0)
        def _():
            a_own(c, h, lambda ref: a_sends(c, h, ref, start))

        @pl.when(a_carries(h))
        def _():
            a_wait(c, h)
            a_sends(c, h, a_there(c, h), start)

    col_turn = jnp.where(
        at_y == 0, 2 * blocks + 2 * (at_x - 1), 3 * blocks + 2 * at_x + 2 * (at_y - 1)
    )

    def col_start(p):
        for h in range(2):

            @pl.when((me_col == 0) & (p == blocks))
            def _():
                a_own(0, h, lambda ref: a_sends(0, h, ref, start, ways=(0, 1)))

            @pl.when((me_col == 0) & (p == 2 * blocks))
            def _():
                a_own(0, h, lambda ref: a_sends(0, h, ref, start, ways=(2, 3), across=False))

    def col_pass(on):
        for h in range(2):

            @pl.when(a_carries(h) & on)
            def _():
                a_wait(0, h)
                a_sends(0, h, a_there(0, h), start)

    def wait_top():
        @pl.when((me_row == plan.rows - 1) & (me_row > 0))
        def _():
            z_copy(0, False).wait_recv()

    def a_turn(p):
        col_start(p)
        col_pass(p == col_turn)

        @pl.when(p == top_turn)
        def _():
            wait_top()

        for h in range(2):
            c = p - top_turn - at_x - at_y

            @pl.when((c >= 0) & (c < top_parts))
            def _():
                a_pass(1 + jnp.clip(c, 0, top_parts - 1), h)

    def a_last():
        col_pass(col_turn >= steps)
        for c in range(top_parts):
            for h in range(2):

                @pl.when(top_turn + c + at_x + at_y >= steps)
                def _():
                    a_pass(1 + c, h)

        if cores == 2:
            for h in range(2):

                @pl.when((me_col != 0) & ((core != h) | (chip == 0)))
                def _():
                    for c in range(1 + top_parts):
                        a_wait(c, h)

        for c in range(1 + top_parts):
            for h in range(2):
                a_sends(c, h, a_there(c, h), sent)

    b_part = squares(m)

    def step(p, carry):
        root = me_row == row_root(p)
        owner = me_col == col_root(p)
        q = jnp.maximum(p - 1, 0)

        @pl.when(p >= SLOTS)
        def _():
            drain(jnp.maximum(p - SLOTS, 0))

        early = blocks
        beside = (chip == col_root(p) // cores) & jnp.logical_not(owner)

        @pl.when(jnp.logical_not(root))
        def _():
            @pl.when(p > 0)
            def _():
                take(q, range(early))

            row_copy(p, 0, True).wait_recv()
            row_sends(p, 0, start)

        @pl.when(root)
        def _():
            @pl.when(p > 0)
            def _():
                take(q, range(1))

            make_rows(p)

            @pl.when(jnp.logical_not(beside))
            def _():
                for i in range(tiles):
                    row_sends(p, i, start)

        @pl.when(owner)
        def _():
            x[...] = pivot_inverse(r[p, p % tiles], SPLIT)

        @pl.when(p > 0)
        def _():
            @pl.when(root)
            def _():
                take(q, range(1, early))

            take(q, range(early, blocks))

        @pl.when(owner)
        def _():
            make_w(p)
            for i in range(blocks):
                w_sends(p, i, start, ways=())
            for i in range(blocks):
                w_sends(p, i, start, across=False)

        @pl.when(jnp.logical_not(root))
        def _():
            for i in range(1, tiles):
                row_copy(p, i, True).wait_recv()
                row_sends(p, i, start)

        @pl.when(p > 0)
        def _():
            update(q)

        @pl.when(root & beside)
        def _():
            for i in range(tiles):
                row_sends(p, i, start)

        if WITH_A:
            z_turn(p)
            a_turn(p)
        return carry

    lax.fori_loop(0, steps, step, 0)
    take(steps - 1, range(blocks))
    update(steps - 1)

    stores = [
        pltpu.make_async_copy(m.at[j], o_ref.at[:, pl.ds(j * PANEL, PANEL)], in_sem.at[j]) for j in range(tiles)
    ]
    for store in stores:
        store.start()

    in_row[me_row, 0] = b_part
    in_row[me_row, 1] = squares(m)
    for d in range(1, plan.rows):
        place = in_row.at[me_row]
        remote(place, place, sum_row_send.at[d], sum_row_recv.at[d], to_row((me_row + d) % plan.rows)).start()
    for d in range(1, plan.rows):
        place = in_row.at[(me_row + plan.rows - d) % plan.rows]
        remote(place, place, sum_row_send.at[d], sum_row_recv.at[d], to_row((me_row + d) % plan.rows)).wait_recv()
    in_col[me_col] = jnp.sum(in_row[...], axis=0)
    for d in range(1, plan.cols):
        place = in_col.at[me_col]
        remote(place, place, sum_col_send.at[d], sum_col_recv.at[d], to_col((me_col + d) % plan.cols)).start()
    for d in range(1, plan.cols):
        place = in_col.at[(me_col + plan.cols - d) % plan.cols]
        remote(place, place, sum_col_send.at[d], sum_col_recv.at[d], to_col((me_col + d) % plan.cols)).wait_recv()
    sums_ref[...] = jnp.sum(in_col[...], axis=0)

    if WITH_A:
        a_last()

        @pl.when(me_row < plan.rows - 1)
        def _():
            for i in range(len(pieces)):
                z_copy(i, False).wait_send()

        @pl.when((me_row == plan.rows - 1) & (me_row > 0))
        def _():
            for i in range(1, len(pieces)):
                z_copy(i, False).wait_recv()

    for d in range(1, plan.rows):
        place = in_row.at[me_row]
        remote(place, place, sum_row_send.at[d], sum_row_recv.at[d], to_row((me_row + d) % plan.rows)).wait_send()
    for d in range(1, plan.cols):
        place = in_col.at[me_col]
        remote(place, place, sum_col_send.at[d], sum_col_recv.at[d], to_col((me_col + d) % plan.cols)).wait_send()

    def row_drain(p, carry):
        for i in range(tiles):
            row_sends(p, i, sent)
        return carry

    lax.fori_loop(0, steps, row_drain, 0)
    lax.fori_loop(steps - SLOTS, steps, lambda p, carry: (drain(p), carry)[1], 0)
    for store in stores:
        store.wait()


WITH_A = True


def sweep_b(plan, matrix, a_matrix, c_matrix):
    height, width = matrix.shape
    tiles = width // PANEL
    blocks = height // PANEL
    steps = STEPS_B
    wide_a = STEPS_A * PANEL
    a_cols, c_cols = a_matrix.shape[1], c_matrix.shape[1]
    pieces = [("a", 0, wide_a)]
    if a_cols > wide_a:
        pieces.append(("a", wide_a, a_cols))
    pieces.append(("c", 0, c_cols))
    assert blocks * (plan.rows - 1) + len(pieces) - 2 < steps
    assert wide_a <= min(a_matrix.shape)
    dma = pltpu.SemaphoreType.DMA
    parts = 1 + wide_a // PANEL
    vmem = pltpu.VMEM
    return pl.pallas_call(
        functools.partial(sweep_kernel, plan, steps, wide_a, pieces),
        out_shape=[
            jax.ShapeDtypeStruct((height, width), jnp.float32),
            jax.ShapeDtypeStruct((2, 8, 128), jnp.float32),
            jax.ShapeDtypeStruct((wide_a, a_cols), jnp.float32),
            jax.ShapeDtypeStruct((wide_a, c_cols), jnp.float32),
            jax.ShapeDtypeStruct((a_matrix.shape[0] + wide_a, wide_a), jnp.float32),
        ],
        in_specs=[pl.BlockSpec(memory_space=pl.ANY)] * 3,
        out_specs=[
            pl.BlockSpec(memory_space=pl.ANY),
            pl.BlockSpec(memory_space=pltpu.VMEM),
        ]
        + [pl.BlockSpec(memory_space=pl.ANY)] * 3,
        scratch_shapes=[
            vmem((tiles, height, PANEL), jnp.float32),
            vmem((steps, height, PANEL), jnp.float32),
            vmem((steps, tiles, PANEL, PANEL), jnp.float32),
            vmem((PANEL, PANEL), jnp.float32),
            vmem((height, PANEL), jnp.float32),
            vmem((plan.rows, 2, 8, 128), jnp.float32),
            vmem((plan.cols, 2, 8, 128), jnp.float32),
            dma((tiles,)),
            dma((steps, tiles)),
            dma((steps, tiles)),
            dma((steps, tiles)),
            dma((steps, blocks)),
            dma((4, SLOTS, blocks)),
            dma((SLOTS, blocks)),
            dma((len(pieces),)),
            dma((len(pieces),)),
            dma((parts, 2)),
            dma((4, parts, 2)),
            dma((parts, 2)),
            dma((plan.rows,)),
            dma((plan.rows,)),
            dma((plan.cols,)),
            dma((plan.cols,)),
        ],
        compiler_params=pltpu.CompilerParams(
            collective_id=0, has_side_effects=True, vmem_limit_bytes=56 * 1024 * 1024
        ),
        name="sweep_b",
    )(matrix, a_matrix, c_matrix)


def halves(value):
    high = value.astype(jnp.bfloat16)
    return high, (value - high.astype(jnp.float32)).astype(jnp.bfloat16)


def finish_kernel(
    wide_a, tile, a_any, c_any, ar_any, cr_any, ac_any, sums, a_blk, c_blk, b_blk, inv_blk, ao_blk, co_blk, bo_blk,
    col, rows, top, w, rows3, w3, sem,
):
    me_row = lax.axis_index("row")
    me_col = lax.axis_index("col")
    a_cols = a_blk.shape[1]
    count = wide_a // PANEL
    here = pl.program_id(0)

    def part(s):
        return pl.ds(s * PANEL, PANEL)

    @pl.when(here == 0)
    def _():
        top_row, left = me_row == 0, me_col == 0

        def fetch(on, src, dst, i):
            @pl.when(on)
            def _():
                pltpu.make_async_copy(src, dst, sem.at[i]).start()

        def fetched(dst, i):
            pltpu.make_async_copy(dst, dst, sem.at[i]).wait()

        first = pl.ds(0, wide_a)
        a_part = rows.at[:, pl.ds(0, a_cols)]
        c_part = rows.at[:, pl.ds(a_cols, rows.shape[1] - a_cols)]
        fetch(left & top_row, a_any.at[first, first], top, 0)
        fetch(left & jnp.logical_not(top_row), ar_any.at[:, first], top, 0)
        fetch(jnp.logical_not(left), ac_any.at[pl.ds(a_any.shape[0], wide_a)], top, 0)
        fetch(left, a_any.at[:, first], col, 1)
        fetch(jnp.logical_not(left), ac_any.at[pl.ds(0, a_any.shape[0])], col, 1)
        fetch(top_row, a_any.at[first], a_part, 2)
        fetch(jnp.logical_not(top_row), ar_any, a_part, 2)
        fetch(top_row, c_any.at[first], c_part, 3)
        fetch(jnp.logical_not(top_row), cr_any, c_part, 3)
        fetched(top, 0)
        for s in range(count):
            inverse = pivot_inverse(top[part(s), part(s)], SPLIT)
            top[part(s), part(s)] = top[part(s), part(s)] - unit()
            if s == 0:
                for i, dst in ((1, col), (2, a_part), (3, c_part)):
                    fetched(dst, i)

            @pl.when(top_row)
            def _():
                col[part(s), part(s)] = col[part(s), part(s)] - unit()

            w[:, part(s)] = dot(col[:, part(s)], inverse, SPLIT)

            @pl.when(left)
            def _():
                rows[:, part(s)] = jnp.zeros((wide_a, PANEL), jnp.float32)
                rows[part(s), part(s)] = unit()

            for later in range(s + 1, count):
                near = dot(top[part(later), part(s)], inverse, SPLIT)
                rows[part(later), :] = rows[part(later), :] - dot(near, rows[part(s), :], SPLIT)
                col[:, part(later)] = col[:, part(later)] - dot(w[:, part(s)], top[part(s), part(later)], SPLIT)
                for after in range(s + 1, count):
                    top[part(later), part(after)] = top[part(later), part(after)] - dot(
                        near, top[part(s), part(after)], SPLIT
                    )

        high, low = halves(rows[...])
        rows3[:wide_a], rows3[wide_a : 2 * wide_a], rows3[2 * wide_a :] = high, low, high
        high, low = halves(w[...])
        w3[:, :wide_a], w3[:, wide_a : 2 * wide_a], w3[:, 2 * wide_a :] = high, high, low

    b_squares = jnp.sum(jnp.sum(sums[0], axis=1, keepdims=True), axis=0, keepdims=True)
    inv_squares = jnp.sum(jnp.sum(sums[1], axis=1, keepdims=True), axis=0, keepdims=True)
    scale = jnp.sqrt(jnp.sqrt(inv_squares / b_squares))
    bo_blk[...] = 0.5 * (scale * b_blk[...] + inv_blk[...] / scale)

    mine = pl.ds(pl.multiple_of(here * tile, tile), tile)
    taken = jnp.dot(w3[mine, :], rows3[...], preferred_element_type=jnp.float32)
    ao_blk[...] = a_blk[...] - taken[:, :a_cols]
    co_blk[...] = c_blk[...] - taken[:, a_cols:]

    @pl.when(me_col == 0)
    def _():
        down = lax.broadcasted_iota(jnp.int32, (tile, wide_a), 0) + here * tile + me_row * a_any.shape[0]
        across = lax.broadcasted_iota(jnp.int32, (tile, wide_a), 1)
        ao_blk[:, :wide_a] = (down == across).astype(jnp.float32) - taken[:, :wide_a]


def finish_all(a_matrix, c_matrix, b_matrix, a_rows, c_rows, a_cols, b_inverse, sums):
    height, width = a_matrix.shape
    c_width = c_matrix.shape[1]
    wide_a = a_cols.shape[1]
    tile = min(2 * PANEL, height)
    count = height // tile
    b_height, b_width = b_matrix.shape
    a_spec = pl.BlockSpec((tile, width), lambda i: (i, 0))
    c_spec = pl.BlockSpec((tile, c_width), lambda i: (i, 0))
    b_spec = pl.BlockSpec((b_height // count, b_width), lambda i: (i, 0))
    return pl.pallas_call(
        functools.partial(finish_kernel, wide_a, tile),
        grid=(count,),
        out_shape=[
            jax.ShapeDtypeStruct((height, width), jnp.float32),
            jax.ShapeDtypeStruct((height, c_width), jnp.float32),
            jax.ShapeDtypeStruct((b_height, b_width), jnp.float32),
        ],
        in_specs=[pl.BlockSpec(memory_space=pl.ANY)] * 5
        + [pl.BlockSpec(memory_space=pltpu.VMEM), a_spec, c_spec, b_spec, b_spec],
        out_specs=[a_spec, c_spec, b_spec],
        scratch_shapes=[
            pltpu.VMEM((height, wide_a), jnp.float32),
            pltpu.VMEM((wide_a, width + c_width), jnp.float32),
            pltpu.VMEM((wide_a, wide_a), jnp.float32),
            pltpu.VMEM((height, wide_a), jnp.float32),
            pltpu.VMEM((3 * wide_a, width + c_width), jnp.bfloat16),
            pltpu.VMEM((height, 3 * wide_a), jnp.bfloat16),
            pltpu.SemaphoreType.DMA((4,)),
        ],
        compiler_params=pltpu.CompilerParams(vmem_limit_bytes=62 * 1024 * 1024),
        name="finish_all",
    )(a_matrix, c_matrix, a_rows, c_rows, a_cols, sums, a_matrix, c_matrix, b_matrix, b_inverse)


def body(plan, a_matrix, b_matrix, c_matrix):
    b_inverse, sums, a_rows, c_rows, a_cols = sweep_b(plan, b_matrix, a_matrix, c_matrix)
    return tuple(finish_all(a_matrix, c_matrix, b_matrix, a_rows, c_rows, a_cols, b_inverse, sums))


def solution(mesh):
    return jax.shard_map(
        functools.partial(body, Plan(mesh)),
        mesh=mesh,
        in_specs=(P("row", "col"), P("row", "col"), P("row", "col")),
        out_specs=(P("row", "col"), P("row", "col"), P("row", "col")),
        check_vma=False,
    )
```

```python
import functools

import jax
import jax.numpy as jnp
from jax import lax
from jax.experimental import pallas as pl
from jax.experimental.pallas import tpu as pltpu
from jax.sharding import PartitionSpec as P

PANEL = 256
PIVOT_ITERS = 6
STEPS_A = 2
STEPS_B = 16

EXACT = lax.Precision.HIGHEST
SPLIT = lax.Precision.HIGH

def dot(x, y, precision):
    return jnp.dot(x, y, precision=precision, preferred_element_type=jnp.float32)


def pivot_inverse(pivot, precision):
    order = pivot.shape[0]
    down = lax.broadcasted_iota(jnp.int32, (order, order), 0)
    across = lax.broadcasted_iota(jnp.int32, (order, order), 1)
    eye = (down == across).astype(jnp.float32)
    kept = pivot * eye
    tall = 1.0 / jnp.sqrt(jnp.sum(kept, axis=1, keepdims=True))
    wide = 1.0 / jnp.sqrt(jnp.sum(kept, axis=0, keepdims=True))
    unit = pivot * tall * wide
    ceiling = jnp.max(jnp.sum(jnp.abs(unit), axis=1, keepdims=True), axis=0, keepdims=True)
    power = eye - unit / ceiling
    total = eye + power
    power = dot(power, power, precision)
    for turn in range(1, PIVOT_ITERS - 1):
        both = dot(power, jnp.concatenate([power, total], 1), precision)
        total = total + both[:, order:]
        power = both[:, :order]
    total = total + dot(power, total, precision)
    return total / ceiling * tall * wide


class Plan:
    def __init__(self, mesh):
        self.rows = mesh.shape["row"]
        self.cols = mesh.shape["col"]
        line = list(mesh.devices.reshape(self.rows, self.cols)[0])
        at = [tuple(getattr(device, "coords", (place, 0, 0))) for place, device in enumerate(line)]
        paired = self.cols % 2 == 0 and all(at[2 * i] == at[2 * i + 1] for i in range(self.cols // 2))
        self.cores = 2 if paired else 1
        chips = at[:: self.cores]
        wide = len({chip[0] for chip in chips})
        tall = len({chip[1] for chip in chips})
        low_x, low_y = min(chip[0] for chip in chips), min(chip[1] for chip in chips)
        plane = [(x + low_x, y + low_y) for y in range(tall) for x in range(wide)]
        if [(chip[0], chip[1]) for chip in chips] != plane:
            wide, tall = len(chips), 1
        self.wide, self.tall = wide, tall


SLOTS = 4
WAYS = ((1, 0), (-1, 0), (0, 1), (0, -1))


def unit():
    down = lax.broadcasted_iota(jnp.int32, (PANEL, PANEL), 0)
    across = lax.broadcasted_iota(jnp.int32, (PANEL, PANEL), 1)
    return (down == across).astype(jnp.float32)


def squares(m):
    total = jnp.zeros((8, 128), jnp.float32)
    for j in range(m.shape[0]):
        value = m[j]
        folded = jnp.sum((value * value).reshape(-1, 8, PANEL), axis=0)
        total = total + folded[:, :128] + folded[:, 128:]
    return total


def sweep_kernel(
    plan, steps, wide_a, pieces,
    b_ref, a_ref, c_ref,
    o_ref, sums_ref, ar_ref, cr_ref, ac_ref,
    m, w, r, x, t, in_row, in_col,
    in_sem, row_recv, row_up, row_down, w_recv, w_send, w_pair,
    z_recv, z_send, ac_recv, ac_send, ac_pair,
    sum_row_recv, sum_row_send, sum_col_recv, sum_col_send,
):
    tiles, height, _ = m.shape
    blocks = height // PANEL
    square = plan.wide == 2 and plan.tall == 2
    kinds = ("xy", "yx")
    me_row = lax.axis_index("row")
    me_col = lax.axis_index("col")
    cores = plan.cores
    chip = me_col // cores
    core = me_col % cores
    pair = chip * cores + (cores - 1 - core)
    at_x, at_y = chip % plan.wide, chip // plan.wide

    def to_row(place):
        return {"row": place, "col": me_col}

    def to_col(place):
        return {"row": me_row, "col": place}

    def remote(src, dst, send, recv, target):
        return pltpu.make_async_remote_copy(
            src_ref=src, dst_ref=dst, send_sem=send, recv_sem=recv,
            device_id=target, device_id_type=pl.DeviceIdType.MESH,
        )

    loads = [
        pltpu.make_async_copy(b_ref.at[:, pl.ds(j * PANEL, PANEL)], m.at[j], in_sem.at[j]) for j in range(tiles)
    ]
    for load in loads:
        load.start()

    barrier = pltpu.get_barrier_semaphore()
    for d in range(1, plan.rows):
        pl.semaphore_signal(
            barrier, inc=1, device_id=to_row((me_row + d) % plan.rows), device_id_type=pl.DeviceIdType.MESH
        )
    for d in range(1, plan.cols):
        pl.semaphore_signal(
            barrier, inc=1, device_id=to_col((me_col + d) % plan.cols), device_id_type=pl.DeviceIdType.MESH
        )
    pl.semaphore_wait(barrier, plan.rows + plan.cols - 2)
    for load in loads:
        load.wait()

    def row_root(p):
        return p // blocks

    def col_root(p):
        return p // tiles

    def row_copy(p, i, up):
        part = r.at[p, (p + i) % tiles]
        sem = (row_up if up else row_down).at[p, i]
        return remote(part, part, sem, row_recv.at[p, i], to_row(me_row + 1 if up else me_row - 1))

    def row_sends(p, i, act):
        @pl.when((me_row >= row_root(p)) & (me_row < plan.rows - 1))
        def _():
            act(row_copy(p, i, True))

        @pl.when((me_row <= row_root(p)) & (me_row > 0))
        def _():
            act(row_copy(p, i, False))

    def routes(root, kind, h):
        at = root // cores
        from_x, from_y = at % plan.wide, at // plan.wide
        carry = me_col == root
        if cores == 2:
            carry = carry | ((chip != at) & (core == h))
        else:
            carry = carry | (me_col != root)
        aside, apart = at_x != from_x, at_y != from_y
        found = []
        for way, (dx, dy) in enumerate(WAYS):
            span, place, origin = (plan.wide, at_x, from_x) if dx else (plan.tall, at_y, from_y)
            if span == 1:
                continue
            if kind in ("xy", "yx"):
                on = (place >= origin) & (place < span - 1) if dx + dy > 0 else (place <= origin) & (place > 0)
                if dx and kind == "xy":
                    on = on & jnp.logical_not(apart)
                if dy and kind == "yx":
                    on = on & jnp.logical_not(aside)
            else:
                on = place < span - 1 if dx + dy > 0 else place > 0
                same = aside == apart
                if kind == "ring x":
                    on = on & (same if dx else aside & jnp.logical_not(apart))
                else:
                    on = on & (same if dy else apart & jnp.logical_not(aside))
            target = (chip + dx + dy * plan.wide) * cores + (h if cores == 2 else 0)
            found.append((way, carry & on, target))
        return carry, found

    def panel_sends(root, kind, h, src, dst, recv, send, couple, act, ways=(0, 1, 2, 3), across=True):
        carry, found = routes(root, kind, h)
        for way, on, target in found:
            if way not in ways:
                continue

            @pl.when(on)
            def _():
                act(remote(src, dst, send(way), recv, to_col(target)))

        if cores == 2 and across:

            @pl.when(carry)
            def _():
                act(remote(src, dst, couple, recv, to_col(pair)))

    def piece(p, i):
        return w.at[p, pl.ds(pl.multiple_of(((p + 1 + i) % blocks) * PANEL, PANEL), PANEL)]

    def w_sends(p, i, act, **which):
        slot = p % SLOTS
        part = piece(p, i)
        panel_sends(
            col_root(p), kinds[i % len(kinds)], i % 2, part, part, w_recv.at[p, i],
            lambda way: w_send.at[way, slot, i], w_pair.at[slot, i], act, **which,
        )

    def w_wait(p, i):
        remote(piece(p, i), piece(p, i), w_pair.at[0, 0], w_recv.at[p, i], to_col(pair)).wait_recv()

    def start(copy):
        copy.start()

    def sent(copy):
        copy.wait_send()

    def take(p, which):
        @pl.when(me_col != col_root(p))
        def _():
            home = chip == col_root(p) // cores
            if cores == 1:
                for i in which:
                    w_wait(p, i)
                    w_sends(p, i, start)
                return
            for h in range(2):

                @pl.when(jnp.logical_not(home) & (core == h))
                def _():
                    for i in which:
                        if i % 2 == h:
                            w_wait(p, i)
                            w_sends(p, i, start)
                    for i in which:
                        if i % 2 != h:
                            w_wait(p, i)

            @pl.when(home)
            def _():
                for i in which:
                    w_wait(p, i)

    def drain(p):
        for i in range(blocks):
            w_sends(p, i, sent)

    def block(p):
        return pl.ds(pl.multiple_of((p % blocks) * PANEL, PANEL), PANEL)

    def make_rows(p):
        for j in range(tiles):
            fresh = m[j, block(p), :]

            @pl.when(p == 0)
            def _():
                r[p, j] = fresh

            @pl.when(p > 0)
            def _():
                q = jnp.maximum(p - 1, 0)
                step = w[q, block(p), :]
                swept = (me_col == col_root(q)) & (q % tiles == j)

                @pl.when(swept)
                def _():
                    r[p, j] = -step

                @pl.when(jnp.logical_not(swept))
                def _():
                    r[p, j] = fresh - dot(step, r[q, j], SPLIT)

    def make_w(p, i):
        j = p % tiles
        mine = block(p + 1 + i)

        @pl.when(p == 0)
        def _():
            t[...] = m[j, mine, :]

        @pl.when(p > 0)
        def _():
            q = jnp.maximum(p - 1, 0)
            t[...] = m[j, mine, :] - dot(w[q, mine, :], r[q, j], SPLIT)

        if i == blocks - 1:

            @pl.when(me_row == row_root(p))
            def _():
                t[...] = t[...] - unit()

        w[p, mine, :] = dot(t[...], x[...], SPLIT)

    def update(q):
        for j in range(tiles):
            swept = (me_col == col_root(q)) & (q % tiles == j)

            @pl.when(swept)
            def _():
                m[j] = -w[q]

                @pl.when(me_row == row_root(q))
                def _():
                    m[j, block(q), :] = unit() - w[q, block(q), :]

            @pl.when(jnp.logical_not(swept))
            def _():
                m[j] = m[j] - dot(w[q], r[q, j], SPLIT)

    def z_copy(i, own):
        kind, low, high = pieces[i]
        there = (ar_ref if kind == "a" else cr_ref).at[:, pl.ds(low, high - low)]
        here = (a_ref if kind == "a" else c_ref).at[pl.ds(0, wide_a), pl.ds(low, high - low)] if own else there
        return remote(here, there, z_send.at[i], z_recv.at[i], to_row(jnp.minimum(me_row + 1, plan.rows - 1)))

    def z_turn(p):
        for i in range(len(pieces)):

            @pl.when((p == blocks * (me_row + 1) - 1 + i) & (me_row < plan.rows - 1))
            def _():
                @pl.when(me_row == 0)
                def _():
                    z_copy(i, True).start()

                @pl.when(me_row > 0)
                def _():
                    z_copy(i, False).wait_recv()
                    z_copy(i, False).start()

    half = PANEL // 2
    top_parts = wide_a // PANEL
    top_turn = steps - 1 - top_parts
    tall_half = a_ref.shape[0] // 2
    first = pl.ds(0, wide_a)

    def a_there(c, h):
        if isinstance(c, int) and c == 0:
            return ac_ref.at[pl.ds(h * tall_half, tall_half)]
        return ac_ref.at[pl.ds(pl.multiple_of(2 * tall_half + (c - 1) * PANEL + h * half, half), half)]

    def a_own(c, h, act):
        if isinstance(c, int) and c == 0:
            act(a_ref.at[pl.ds(h * tall_half, tall_half), first])
            return
        spot = pl.ds(pl.multiple_of((c - 1) * PANEL + h * half, half), half)

        @pl.when(me_row == 0)
        def _():
            act(a_ref.at[spot, first])

        @pl.when(me_row > 0)
        def _():
            act(ar_ref.at[spot, first])

    def a_sends(c, h, src, act, **which):
        kind = "xy" if isinstance(c, int) and c == 0 else ("xy", "yx")[h]
        panel_sends(
            jnp.int32(0), kind, h, src, a_there(c, h), ac_recv.at[c, h],
            lambda way: ac_send.at[way, c, h], ac_pair.at[c, h], act, **which,
        )

    def a_wait(c, h):
        part = a_there(c, h)
        remote(part, part, ac_pair.at[c, h], ac_recv.at[c, h], to_col(pair)).wait_recv()

    def a_carries(h):
        return (chip != 0) & ((core == h) | (cores == 1))

    def a_pass(c, h):
        @pl.when(me_col == 0)
        def _():
            a_own(c, h, lambda ref: a_sends(c, h, ref, start))

        @pl.when(a_carries(h))
        def _():
            a_wait(c, h)
            a_sends(c, h, a_there(c, h), start)

    col_turn = jnp.where(
        at_y == 0, 2 * blocks + 2 * (at_x - 1), 3 * blocks + 2 * at_x + 2 * (at_y - 1)
    )

    def col_start(p):
        for h in range(2):

            @pl.when((me_col == 0) & (p == blocks))
            def _():
                a_own(0, h, lambda ref: a_sends(0, h, ref, start, ways=(0, 1)))

            @pl.when((me_col == 0) & (p == 2 * blocks))
            def _():
                a_own(0, h, lambda ref: a_sends(0, h, ref, start, ways=(2, 3), across=False))

    def col_pass(on):
        for h in range(2):

            @pl.when(a_carries(h) & on)
            def _():
                a_wait(0, h)
                a_sends(0, h, a_there(0, h), start)

    def wait_top():
        @pl.when((me_row == plan.rows - 1) & (me_row > 0))
        def _():
            z_copy(0, False).wait_recv()

    def a_turn(p):
        col_start(p)
        col_pass(p == col_turn)

        @pl.when(p == top_turn)
        def _():
            wait_top()

        for h in range(2):
            c = p - top_turn - at_x - at_y

            @pl.when((c >= 0) & (c < top_parts))
            def _():
                a_pass(1 + jnp.clip(c, 0, top_parts - 1), h)

    def a_last():
        col_pass(col_turn >= steps)
        for c in range(top_parts):
            for h in range(2):

                @pl.when(top_turn + c + at_x + at_y >= steps)
                def _():
                    a_pass(1 + c, h)

        if cores == 2:
            for h in range(2):

                @pl.when((me_col != 0) & ((core != h) | (chip == 0)))
                def _():
                    for c in range(1 + top_parts):
                        a_wait(c, h)

        for c in range(1 + top_parts):
            for h in range(2):
                a_sends(c, h, a_there(c, h), sent)

    b_part = squares(m)

    def step(p, carry):
        root = me_row == row_root(p)
        owner = me_col == col_root(p)
        q = jnp.maximum(p - 1, 0)

        @pl.when(p >= SLOTS)
        def _():
            drain(jnp.maximum(p - SLOTS, 0))

        early = blocks
        beside = (chip == col_root(p) // cores) & jnp.logical_not(owner)

        @pl.when(jnp.logical_not(root))
        def _():
            @pl.when(p > 0)
            def _():
                take(q, range(early))

            row_copy(p, 0, True).wait_recv()
            row_sends(p, 0, start)

        @pl.when(root)
        def _():
            @pl.when(p > 0)
            def _():
                take(q, range(1))

            make_rows(p)

            @pl.when(jnp.logical_not(beside))
            def _():
                for i in range(tiles):
                    row_sends(p, i, start)

        @pl.when(owner)
        def _():
            x[...] = pivot_inverse(r[p, p % tiles], SPLIT)

        @pl.when(p > 0)
        def _():
            @pl.when(root)
            def _():
                take(q, range(1, early))

            take(q, range(early, blocks))

        @pl.when(owner)
        def _():
            for i in range(blocks):
                make_w(p, i)
                w_sends(p, i, start)

        @pl.when(jnp.logical_not(root))
        def _():
            for i in range(1, tiles):
                row_copy(p, i, True).wait_recv()
                row_sends(p, i, start)

        @pl.when(p > 0)
        def _():
            update(q)

        @pl.when(root & beside)
        def _():
            for i in range(tiles):
                row_sends(p, i, start)

        if WITH_A:
            z_turn(p)
            a_turn(p)
        return carry

    lax.fori_loop(0, steps, step, 0)
    take(steps - 1, range(blocks))
    update(steps - 1)

    stores = [
        pltpu.make_async_copy(m.at[j], o_ref.at[:, pl.ds(j * PANEL, PANEL)], in_sem.at[j]) for j in range(tiles)
    ]
    for store in stores:
        store.start()

    in_row[me_row, 0] = b_part
    in_row[me_row, 1] = squares(m)
    for d in range(1, plan.rows):
        place = in_row.at[me_row]
        remote(place, place, sum_row_send.at[d], sum_row_recv.at[d], to_row((me_row + d) % plan.rows)).start()
    for d in range(1, plan.rows):
        place = in_row.at[(me_row + plan.rows - d) % plan.rows]
        remote(place, place, sum_row_send.at[d], sum_row_recv.at[d], to_row((me_row + d) % plan.rows)).wait_recv()
    in_col[me_col] = jnp.sum(in_row[...], axis=0)
    for d in range(1, plan.cols):
        place = in_col.at[me_col]
        remote(place, place, sum_col_send.at[d], sum_col_recv.at[d], to_col((me_col + d) % plan.cols)).start()
    for d in range(1, plan.cols):
        place = in_col.at[(me_col + plan.cols - d) % plan.cols]
        remote(place, place, sum_col_send.at[d], sum_col_recv.at[d], to_col((me_col + d) % plan.cols)).wait_recv()
    sums_ref[...] = jnp.sum(in_col[...], axis=0)

    if WITH_A:
        a_last()

        @pl.when(me_row < plan.rows - 1)
        def _():
            for i in range(len(pieces)):
                z_copy(i, False).wait_send()

        @pl.when((me_row == plan.rows - 1) & (me_row > 0))
        def _():
            for i in range(1, len(pieces)):
                z_copy(i, False).wait_recv()

    for d in range(1, plan.rows):
        place = in_row.at[me_row]
        remote(place, place, sum_row_send.at[d], sum_row_recv.at[d], to_row((me_row + d) % plan.rows)).wait_send()
    for d in range(1, plan.cols):
        place = in_col.at[me_col]
        remote(place, place, sum_col_send.at[d], sum_col_recv.at[d], to_col((me_col + d) % plan.cols)).wait_send()

    def row_drain(p, carry):
        for i in range(tiles):
            row_sends(p, i, sent)
        return carry

    lax.fori_loop(0, steps, row_drain, 0)
    lax.fori_loop(steps - SLOTS, steps, lambda p, carry: (drain(p), carry)[1], 0)
    for store in stores:
        store.wait()


WITH_A = True


def sweep_b(plan, matrix, a_matrix, c_matrix):
    height, width = matrix.shape
    tiles = width // PANEL
    blocks = height // PANEL
    steps = STEPS_B
    wide_a = STEPS_A * PANEL
    a_cols, c_cols = a_matrix.shape[1], c_matrix.shape[1]
    pieces = [("a", 0, wide_a)]
    if a_cols > wide_a:
        pieces.append(("a", wide_a, a_cols))
    pieces.append(("c", 0, c_cols))
    assert blocks * (plan.rows - 1) + len(pieces) - 2 < steps
    assert wide_a <= min(a_matrix.shape)
    dma = pltpu.SemaphoreType.DMA
    parts = 1 + wide_a // PANEL
    vmem = pltpu.VMEM
    return pl.pallas_call(
        functools.partial(sweep_kernel, plan, steps, wide_a, pieces),
        out_shape=[
            jax.ShapeDtypeStruct((height, width), jnp.float32),
            jax.ShapeDtypeStruct((2, 8, 128), jnp.float32),
            jax.ShapeDtypeStruct((wide_a, a_cols), jnp.float32),
            jax.ShapeDtypeStruct((wide_a, c_cols), jnp.float32),
            jax.ShapeDtypeStruct((a_matrix.shape[0] + wide_a, wide_a), jnp.float32),
        ],
        in_specs=[pl.BlockSpec(memory_space=pl.ANY)] * 3,
        out_specs=[
            pl.BlockSpec(memory_space=pl.ANY),
            pl.BlockSpec(memory_space=pltpu.VMEM),
        ]
        + [pl.BlockSpec(memory_space=pl.ANY)] * 3,
        scratch_shapes=[
            vmem((tiles, height, PANEL), jnp.float32),
            vmem((steps, height, PANEL), jnp.float32),
            vmem((steps, tiles, PANEL, PANEL), jnp.float32),
            vmem((PANEL, PANEL), jnp.float32),
            vmem((PANEL, PANEL), jnp.float32),
            vmem((plan.rows, 2, 8, 128), jnp.float32),
            vmem((plan.cols, 2, 8, 128), jnp.float32),
            dma((tiles,)),
            dma((steps, tiles)),
            dma((steps, tiles)),
            dma((steps, tiles)),
            dma((steps, blocks)),
            dma((4, SLOTS, blocks)),
            dma((SLOTS, blocks)),
            dma((len(pieces),)),
            dma((len(pieces),)),
            dma((parts, 2)),
            dma((4, parts, 2)),
            dma((parts, 2)),
            dma((plan.rows,)),
            dma((plan.rows,)),
            dma((plan.cols,)),
            dma((plan.cols,)),
        ],
        compiler_params=pltpu.CompilerParams(
            collective_id=0, has_side_effects=True, vmem_limit_bytes=56 * 1024 * 1024
        ),
        name="sweep_b",
    )(matrix, a_matrix, c_matrix)


def halves(value):
    high = value.astype(jnp.bfloat16)
    return high, (value - high.astype(jnp.float32)).astype(jnp.bfloat16)


def finish_kernel(
    wide_a, tile, a_any, c_any, ar_any, cr_any, ac_any, sums, a_blk, c_blk, b_blk, inv_blk, ao_blk, co_blk, bo_blk,
    col, rows, top, w, rows3, w3, sem,
):
    me_row = lax.axis_index("row")
    me_col = lax.axis_index("col")
    a_cols = a_blk.shape[1]
    count = wide_a // PANEL
    here = pl.program_id(0)

    def part(s):
        return pl.ds(s * PANEL, PANEL)

    @pl.when(here == 0)
    def _():
        top_row, left = me_row == 0, me_col == 0

        def fetch(on, src, dst, i):
            @pl.when(on)
            def _():
                pltpu.make_async_copy(src, dst, sem.at[i]).start()

        def fetched(dst, i):
            pltpu.make_async_copy(dst, dst, sem.at[i]).wait()

        first = pl.ds(0, wide_a)
        a_part = rows.at[:, pl.ds(0, a_cols)]
        c_part = rows.at[:, pl.ds(a_cols, rows.shape[1] - a_cols)]
        fetch(left & top_row, a_any.at[first, first], top, 0)
        fetch(left & jnp.logical_not(top_row), ar_any.at[:, first], top, 0)
        fetch(jnp.logical_not(left), ac_any.at[pl.ds(a_any.shape[0], wide_a)], top, 0)
        fetch(left, a_any.at[:, first], col, 1)
        fetch(jnp.logical_not(left), ac_any.at[pl.ds(0, a_any.shape[0])], col, 1)
        fetch(top_row, a_any.at[first], a_part, 2)
        fetch(jnp.logical_not(top_row), ar_any, a_part, 2)
        fetch(top_row, c_any.at[first], c_part, 3)
        fetch(jnp.logical_not(top_row), cr_any, c_part, 3)
        fetched(top, 0)
        for s in range(count):
            inverse = pivot_inverse(top[part(s), part(s)], SPLIT)
            top[part(s), part(s)] = top[part(s), part(s)] - unit()
            if s == 0:
                for i, dst in ((1, col), (2, a_part), (3, c_part)):
                    fetched(dst, i)

            @pl.when(top_row)
            def _():
                col[part(s), part(s)] = col[part(s), part(s)] - unit()

            w[:, part(s)] = dot(col[:, part(s)], inverse, SPLIT)

            @pl.when(left)
            def _():
                rows[:, part(s)] = jnp.zeros((wide_a, PANEL), jnp.float32)
                rows[part(s), part(s)] = unit()

            for later in range(s + 1, count):
                near = dot(top[part(later), part(s)], inverse, SPLIT)
                rows[part(later), :] = rows[part(later), :] - dot(near, rows[part(s), :], SPLIT)
                col[:, part(later)] = col[:, part(later)] - dot(w[:, part(s)], top[part(s), part(later)], SPLIT)
                for after in range(s + 1, count):
                    top[part(later), part(after)] = top[part(later), part(after)] - dot(
                        near, top[part(s), part(after)], SPLIT
                    )

        high, low = halves(rows[...])
        rows3[:wide_a], rows3[wide_a : 2 * wide_a], rows3[2 * wide_a :] = high, low, high
        high, low = halves(w[...])
        w3[:, :wide_a], w3[:, wide_a : 2 * wide_a], w3[:, 2 * wide_a :] = high, high, low

    b_squares = jnp.sum(jnp.sum(sums[0], axis=1, keepdims=True), axis=0, keepdims=True)
    inv_squares = jnp.sum(jnp.sum(sums[1], axis=1, keepdims=True), axis=0, keepdims=True)
    scale = jnp.sqrt(jnp.sqrt(inv_squares / b_squares))
    bo_blk[...] = 0.5 * (scale * b_blk[...] + inv_blk[...] / scale)

    mine = pl.ds(pl.multiple_of(here * tile, tile), tile)
    taken = jnp.dot(w3[mine, :], rows3[...], preferred_element_type=jnp.float32)
    ao_blk[...] = a_blk[...] - taken[:, :a_cols]
    co_blk[...] = c_blk[...] - taken[:, a_cols:]

    @pl.when(me_col == 0)
    def _():
        down = lax.broadcasted_iota(jnp.int32, (tile, wide_a), 0) + here * tile + me_row * a_any.shape[0]
        across = lax.broadcasted_iota(jnp.int32, (tile, wide_a), 1)
        ao_blk[:, :wide_a] = (down == across).astype(jnp.float32) - taken[:, :wide_a]


def finish_all(a_matrix, c_matrix, b_matrix, a_rows, c_rows, a_cols, b_inverse, sums):
    height, width = a_matrix.shape
    c_width = c_matrix.shape[1]
    wide_a = a_cols.shape[1]
    tile = min(2 * PANEL, height)
    count = height // tile
    b_height, b_width = b_matrix.shape
    a_spec = pl.BlockSpec((tile, width), lambda i: (i, 0))
    c_spec = pl.BlockSpec((tile, c_width), lambda i: (i, 0))
    b_spec = pl.BlockSpec((b_height // count, b_width), lambda i: (i, 0))
    return pl.pallas_call(
        functools.partial(finish_kernel, wide_a, tile),
        grid=(count,),
        out_shape=[
            jax.ShapeDtypeStruct((height, width), jnp.float32),
            jax.ShapeDtypeStruct((height, c_width), jnp.float32),
            jax.ShapeDtypeStruct((b_height, b_width), jnp.float32),
        ],
        in_specs=[pl.BlockSpec(memory_space=pl.ANY)] * 5
        + [pl.BlockSpec(memory_space=pltpu.VMEM), a_spec, c_spec, b_spec, b_spec],
        out_specs=[a_spec, c_spec, b_spec],
        scratch_shapes=[
            pltpu.VMEM((height, wide_a), jnp.float32),
            pltpu.VMEM((wide_a, width + c_width), jnp.float32),
            pltpu.VMEM((wide_a, wide_a), jnp.float32),
            pltpu.VMEM((height, wide_a), jnp.float32),
            pltpu.VMEM((3 * wide_a, width + c_width), jnp.bfloat16),
            pltpu.VMEM((height, 3 * wide_a), jnp.bfloat16),
            pltpu.SemaphoreType.DMA((4,)),
        ],
        compiler_params=pltpu.CompilerParams(vmem_limit_bytes=62 * 1024 * 1024),
        name="finish_all",
    )(a_matrix, c_matrix, a_rows, c_rows, a_cols, sums, a_matrix, c_matrix, b_matrix, b_inverse)


def body(plan, a_matrix, b_matrix, c_matrix):
    b_inverse, sums, a_rows, c_rows, a_cols = sweep_b(plan, b_matrix, a_matrix, c_matrix)
    return tuple(finish_all(a_matrix, c_matrix, b_matrix, a_rows, c_rows, a_cols, b_inverse, sums))


def solution(mesh):
    return jax.shard_map(
        functools.partial(body, Plan(mesh)),
        mesh=mesh,
        in_specs=(P("row", "col"), P("row", "col"), P("row", "col")),
        out_specs=(P("row", "col"), P("row", "col"), P("row", "col")),
        check_vma=False,
    )
```
